1024 devices in a mesh: face: 16 (over z_hi, x), tile: 16 (over y, core), lev: 4 (over z_lo).
Axes of the slice: x: 4, y: 8, z: 16 (z_hi: 4, z_lo: 4; z = z_hi * 4 + z_lo), core: 2. Of those that a mesh axis runs over, the one named last changes fastest.
Arguments:
- airflow_components: float32 [2, 72, 128, 2048], P(None, 'lev', 'face', 'tile'), may hold values from -4.5 to 4.5, as said below
- heat_state: float32 [72, 128, 2048], P('lev', 'face', 'tile'), may hold values from 0.5 to 2
- layer_pressure_depth: float32 [72, 128, 2048], P('lev', 'face', 'tile'), may hold values from 0.5 to 2
- constituent_masses: float32 [18, 72, 128, 2048], P(None, 'lev', 'face', 'tile'), may hold values from 0.1 to 1
- ground_gravity_potential: float32 [128, 2048], P('face', 'tile'), may hold values from -8 to 8
- inverse_mapping_entries: float32 [4, 128, 2048], P(None, 'face', 'tile'), may hold values from -4 to 4
- mapping_determinant: float32 [128, 2048], P('face', 'tile'), may hold values from 0.5 to 2
- interface_rightangle_rotations: int32 [16, 16, 2], replicated, may hold values from 0 to 3
- interface_flipped_markers: int32 [16, 16, 2], replicated, may hold values from 0 to 1
- corner_block_tally: int32 [16, 16], replicated, may hold values from 3 to 4
Outputs:
- airflow_next: float32 [2, 72, 128, 2048], P(None, 'lev', 'face', 'tile')
- heat_state_next: float32 [72, 128, 2048], P('lev', 'face', 'tile')
- pressure_depth_next: float32 [72, 128, 2048], P('lev', 'face', 'tile')
- constituent_masses_next: float32 [18, 72, 128, 2048], P(None, 'lev', 'face', 'tile')
- stepping_bounds: float32 [2], replicated
The draws below stay inside these ranges and needn't reach their ends.
Inputs may be any that keep to these rules, and one draw needn't show every extreme that they name: `airflow_components`: component magnitudes grow across the grid by up to a factor of 9. `interface_rightangle_rotations`: entry [f, t, 0] concerns the boundary between blocks (f, t) and (f+1, t), entry [f, t, 1] the one between (f, t) and (f, t+1). `interface_flipped_markers`: indexed like interface_rightangle_rotations. `corner_block_tally`: entry [f, t] belongs to the corner shared by blocks (f, t), (f+1, t), (f, t+1), (f+1, t+1).
All inputs are finite; a program needn't handle non-finite values.
Results may differ from the reference program's by a relative error of at most 0.00012.
Values sent between devices are 32-bit elements; how exact they have to be, the bound alone decides.
No kernel may reach another device: no remote copies, remote signals or barrier semaphores. Data moves between devices by JAX's collectives and lax.ppermute only.
A program may use at most 32 MiB of HBM per device.

```python
import math
import jax
import jax.numpy as jnp
import numpy as np
from jax import lax

QSIZE = 18
MESH_NODE_NORTHS = 128
MESH_NODE_EASTS = 2048
LAYER_NUMBER = 72
N_FACE = 16
N_TILE = 16


def draw_airflow_components(key, part):
    row_position = jnp.arange(MESH_NODE_NORTHS, dtype=jnp.float32)[:, None] / MESH_NODE_NORTHS
    column_position = jnp.arange(MESH_NODE_EASTS, dtype=jnp.float32)[None, :] / MESH_NODE_EASTS
    spread_factor = 0.5 * jnp.exp(jnp.log(3.0) * (row_position + column_position))
    standard = jnp.clip(jax.random.normal(key, (2, LAYER_NUMBER, MESH_NODE_NORTHS, MESH_NODE_EASTS), jnp.float32), -3.0, 3.0)
    return (standard * spread_factor / 3.0).astype(jnp.float32)


def touch_ends(drawn, stream_key, smallest, largest):
    longest = drawn.shape.index(max(drawn.shape))
    spots = []
    for shift in (0, 1):
        where = [jax.random.randint(jax.random.fold_in(stream_key, axis), (), 0, length) for axis, length in enumerate(drawn.shape)]
        where[longest] = (where[longest] + shift) % drawn.shape[longest]
        spots.append(tuple(where))
    return drawn.at[spots[0]].set(smallest).at[spots[1]].set(largest)


def steps_of(rng, shape, cuts, low, largest):
    def one(position, blocks):
        heights = jax.random.uniform(jax.random.fold_in(jax.random.fold_in(rng, 6), position), (blocks,), jnp.float32, low / len(cuts), largest / len(cuts))
        return jnp.repeat(jnp.exp(heights), shape[position] // blocks).reshape((-1,) + (1,) * (len(shape) - position - 1))

    level = one(*cuts[0])
    for cut in cuts[1:]:
        level = level * one(*cut)
    return level


def noise(key, extent, spread, bound, split=(), kind=jnp.bfloat16):
    result = spread * jax.random.normal(key, extent, jnp.float32)
    if split:
        result = result * steps_of(key, extent, split, -0.22, 0.18)
    return jnp.clip(result, -bound, bound).astype(kind)


def setup_inputs(seed: int = 0) -> dict:
    splits = jax.random.split(jax.random.key(seed), 11)
    airflow_components = draw_airflow_components(jax.random.fold_in(splits[10], 71), 0)
    heat_state = jnp.clip(jnp.exp(math.log(2.0) - 1.3862944 * jax.random.uniform(splits[1], (LAYER_NUMBER, MESH_NODE_NORTHS, MESH_NODE_EASTS), jnp.float32) ** steps_of(splits[1], (LAYER_NUMBER, MESH_NODE_NORTHS, MESH_NODE_EASTS), ((0, 4), (1, 16), (2, 16)), -0.2, 0.2)), 0.5, 2.0)
    layer_pressure_depth = jnp.clip(jnp.exp(math.log(2.0) - 1.3862944 * jax.random.uniform(splits[2], (LAYER_NUMBER, MESH_NODE_NORTHS, MESH_NODE_EASTS), jnp.float32) ** steps_of(splits[2], (LAYER_NUMBER, MESH_NODE_NORTHS, MESH_NODE_EASTS), ((0, 4), (1, 16), (2, 16)), -0.2, 0.2)), 0.5, 2.0)
    constituent_masses = jnp.clip(jnp.exp(math.log(1.0) - 2.3025851 * jax.random.uniform(splits[3], (QSIZE, LAYER_NUMBER, MESH_NODE_NORTHS, MESH_NODE_EASTS), jnp.float32) ** steps_of(splits[3], (QSIZE, LAYER_NUMBER, MESH_NODE_NORTHS, MESH_NODE_EASTS), ((1, 4), (2, 16), (3, 16)), -0.2, 0.2)), 0.1, 1.0)
    ground_gravity_potential = noise(splits[4], (MESH_NODE_NORTHS, MESH_NODE_EASTS), 2.0, 8.0, ((0, 16), (1, 16)), jnp.float32)
    inverse_mapping_entries = noise(splits[5], (4, MESH_NODE_NORTHS, MESH_NODE_EASTS), 1.0, 4.0, ((1, 16), (2, 16)), jnp.float32)
    mapping_determinant = jnp.clip(jnp.exp(math.log(2.0) - 1.3862944 * jax.random.uniform(splits[6], (MESH_NODE_NORTHS, MESH_NODE_EASTS), jnp.float32) ** steps_of(splits[6], (MESH_NODE_NORTHS, MESH_NODE_EASTS), ((0, 16), (1, 16)), -0.2, 0.2)), 0.5, 2.0)
    interface_rightangle_rotations = touch_ends(jax.random.randint(splits[7], (N_FACE, N_TILE, 2), 0, 4), jax.random.fold_in(splits[7], 1), 0, 3).astype(jnp.int32)
    interface_flipped_markers = touch_ends(jax.random.randint(splits[8], (N_FACE, N_TILE, 2), 0, 2), jax.random.fold_in(splits[8], 1), 0, 1).astype(jnp.int32)
    corner_block_tally = touch_ends(jax.random.randint(splits[9], (N_FACE, N_TILE), 3, 5), jax.random.fold_in(splits[9], 1), 3, 4).astype(jnp.int32)
    return dict(airflow_components=airflow_components, heat_state=heat_state, layer_pressure_depth=layer_pressure_depth, constituent_masses=constituent_masses, ground_gravity_potential=ground_gravity_potential, inverse_mapping_entries=inverse_mapping_entries, mapping_determinant=mapping_determinant, interface_rightangle_rotations=interface_rightangle_rotations, interface_flipped_markers=interface_flipped_markers, corner_block_tally=corner_block_tally)


time_step = 0.05
viscosity = 0.05
highest = lax.Precision.HIGHEST

def gll_tables():
    offset = 1.0 / math.sqrt(5.0)
    gll_nodes = np.array([-1.0, -offset, offset, 1.0])
    weights = np.array([1.0 / 6.0, 5.0 / 6.0, 5.0 / 6.0, 1.0 / 6.0])
    barycentric = np.ones(4)
    for outer_index in range(4):
        for inner_index in range(4):
            if inner_index != outer_index:
                barycentric[outer_index] = barycentric[outer_index] / (gll_nodes[outer_index] - gll_nodes[inner_index])
    derivative = np.zeros((4, 4))
    for outer_index in range(4):
        for inner_index in range(4):
            if inner_index != outer_index:
                derivative[outer_index, inner_index] = barycentric[inner_index] / barycentric[outer_index] / (gll_nodes[outer_index] - gll_nodes[inner_index])
        derivative[outer_index, outer_index] = -np.sum(derivative[outer_index])
    return (derivative, weights)

def advance(east_wind, north_wind, temp_field, thick_field, tracer_field, geo_field, inverse_mapping_entries, mapping_determinant, along_rows, along_columns):

    def gradient(scalar):
        first_part = along_rows(scalar)
        second_part = along_columns(scalar)
        return (inverse_mapping_entries[0] * first_part + inverse_mapping_entries[2] * second_part, inverse_mapping_entries[1] * first_part + inverse_mapping_entries[3] * second_part)

    def divergence(east_part, north_part):
        first_flux = mapping_determinant * (inverse_mapping_entries[0] * east_part + inverse_mapping_entries[1] * north_part)
        second_flux = mapping_determinant * (inverse_mapping_entries[2] * east_part + inverse_mapping_entries[3] * north_part)
        return (along_rows(first_flux) + along_columns(second_flux)) / mapping_determinant
    energy = 0.5 * (east_wind * east_wind + north_wind * north_wind) + geo_field
    energy_x, energy_y = gradient(energy)
    temp_x, temp_y = gradient(temp_field)
    thick_x, thick_y = gradient(thick_field)
    laplace = divergence(thick_x, thick_y)
    new_east = east_wind - time_step * energy_x
    new_north = north_wind - time_step * energy_y
    new_temp = temp_field - time_step * (east_wind * temp_x + north_wind * temp_y)
    new_thick = thick_field - time_step * divergence(thick_field * east_wind, thick_field * north_wind) + time_step * viscosity * laplace
    new_tracer = tracer_field - time_step * divergence(tracer_field * east_wind, tracer_field * north_wind)
    spacing = jnp.sqrt(inverse_mapping_entries[0] * inverse_mapping_entries[0] + inverse_mapping_entries[1] * inverse_mapping_entries[1] + inverse_mapping_entries[2] * inverse_mapping_entries[2] + inverse_mapping_entries[3] * inverse_mapping_entries[3])
    courant = jnp.max(time_step * jnp.sqrt(east_wind * east_wind + north_wind * north_wind) * spacing)
    damping = jnp.max(time_step * viscosity * jnp.abs(laplace))
    fields = jnp.concatenate([new_east[None], new_north[None], new_temp[None], new_thick[None], new_tracer], 0)
    return (fields, courant, damping)

def turn(pieces, code):
    cosine = jnp.where(code == 0, 1.0, jnp.where(code == 2, -1.0, 0.0)).astype(jnp.float32)
    sine = jnp.where(code == 1, 1.0, jnp.where(code == 3, -1.0, 0.0)).astype(jnp.float32)
    first_part = cosine * pieces[0] - sine * pieces[1]
    second_part = sine * pieces[0] + cosine * pieces[1]
    return jnp.concatenate([first_part[None], second_part[None], pieces[2:]], 0)

def flip_edge(strip, flag):
    return jnp.where(flag[..., None] == 1, strip[..., ::-1], strip)

def fix_edge(strip, flag, code):
    return turn(flip_edge(strip, flag), code[..., None])

def assemble(inner, top_rim, bottom_rim, left_rim, right_rim, corner_ll, corner_lh, corner_hl, corner_hh):
    first_row = jnp.concatenate([corner_ll[..., None], top_rim, corner_lh[..., None]], -1)
    last_row = jnp.concatenate([corner_hl[..., None], bottom_rim, corner_hh[..., None]], -1)
    middle = jnp.concatenate([left_rim[..., None], inner, right_rim[..., None]], -1)
    return jnp.concatenate([first_row[..., None, :], middle, last_row[..., None, :]], -2)

def shared_sums(padded):
    row_count = padded.shape[-2] - 2
    column_count = padded.shape[-1] - 2
    row_low = (jnp.arange(row_count) % 4 == 0)[:, None]
    row_high = (jnp.arange(row_count) % 4 == 3)[:, None]
    across = padded[..., 1:-1, :] + jnp.where(row_low, padded[..., :-2, :], 0.0) + jnp.where(row_high, padded[..., 2:, :], 0.0)
    column_low = jnp.arange(column_count) % 4 == 0
    column_high = jnp.arange(column_count) % 4 == 3
    return across[..., 1:-1] + jnp.where(column_low, across[..., :-2], 0.0) + jnp.where(column_high, across[..., 2:], 0.0)

def combine_block(pieces, mass_pieces, rotations, flips, valences):
    inner, top_rim, bottom_rim, left_rim, right_rim, corner_ll, corner_lh, corner_hl, corner_hh = pieces
    mass_inner, mass_top, mass_bottom, mass_left, mass_right, mass_ll, mass_lh, mass_hl, mass_hh = mass_pieces
    top_code, bottom_code, left_code, right_code = rotations
    top_flag, bottom_flag, left_flag, right_flag = flips
    valence_ll, valence_lh, valence_hl, valence_hh = valences
    fixed = assemble(inner, fix_edge(top_rim, top_flag, top_code), fix_edge(bottom_rim, bottom_flag, bottom_code), fix_edge(left_rim, left_flag, left_code), fix_edge(right_rim, right_flag, right_code), jnp.where(valence_ll == 4, turn(corner_ll, (top_code + left_code) % 4), 0.0), jnp.where(valence_lh == 4, turn(corner_lh, (top_code + right_code) % 4), 0.0), jnp.where(valence_hl == 4, turn(corner_hl, (bottom_code + left_code) % 4), 0.0), jnp.where(valence_hh == 4, turn(corner_hh, (bottom_code + right_code) % 4), 0.0))
    mass_fixed = assemble(mass_inner, flip_edge(mass_top, top_flag), flip_edge(mass_bottom, bottom_flag), flip_edge(mass_left, left_flag), flip_edge(mass_right, right_flag), jnp.where(valence_ll == 4, mass_ll, 0.0), jnp.where(valence_lh == 4, mass_lh, 0.0), jnp.where(valence_hl == 4, mass_hl, 0.0), jnp.where(valence_hh == 4, mass_hh, 0.0))
    return shared_sums(fixed) / shared_sums(mass_fixed)

def block_pieces(field, face_count, tile_count):
    field_count = field.shape[0]
    row_count = field.shape[1] // face_count
    column_count = field.shape[2] // tile_count
    blocks = field.reshape(field_count, face_count, row_count, tile_count, column_count).transpose(0, 1, 3, 2, 4)
    top_rim = jnp.roll(blocks[:, :, :, -1, :], 1, axis=1)
    bottom_rim = jnp.roll(blocks[:, :, :, 0, :], -1, axis=1)
    left_rim = jnp.roll(blocks[:, :, :, :, -1], 1, axis=2)
    right_rim = jnp.roll(blocks[:, :, :, :, 0], -1, axis=2)
    corner_ll = jnp.roll(jnp.roll(blocks[:, :, :, -1, -1], 1, axis=1), 1, axis=2)
    corner_lh = jnp.roll(jnp.roll(blocks[:, :, :, -1, 0], 1, axis=1), -1, axis=2)
    corner_hl = jnp.roll(jnp.roll(blocks[:, :, :, 0, -1], -1, axis=1), 1, axis=2)
    corner_hh = jnp.roll(jnp.roll(blocks[:, :, :, 0, 0], -1, axis=1), -1, axis=2)
    return (blocks, top_rim, bottom_rim, left_rim, right_rim, corner_ll, corner_lh, corner_hl, corner_hh)

def reference(airflow_components, heat_state, layer_pressure_depth, constituent_masses, ground_gravity_potential, inverse_mapping_entries, mapping_determinant, interface_rightangle_rotations, interface_flipped_markers, corner_block_tally):
    derivative, weights = gll_tables()
    deriv_table = jnp.asarray(derivative, jnp.float32)

    def along_rows(field):
        field_shape = field.shape
        blocks = field.reshape(field_shape[:-2] + (field_shape[-2] // 4, 4, field_shape[-1]))
        return jnp.einsum('ab,...ebc->...eac', deriv_table, blocks, precision=highest).reshape(field_shape)

    def along_columns(field):
        field_shape = field.shape
        blocks = field.reshape(field_shape[:-1] + (field_shape[-1] // 4, 4))
        return jnp.einsum('ab,...eb->...ea', deriv_table, blocks, precision=highest).reshape(field_shape)
    strip_parts_sequence = heat_state * layer_pressure_depth
    column_total = lax.optimization_barrier(jnp.sum(strip_parts_sequence, axis=0))
    gravity_potential_altitude = ground_gravity_potential + (column_total - jnp.cumsum(strip_parts_sequence, axis=0)) + 0.5 * strip_parts_sequence
    grid_rows = mapping_determinant.shape[0]
    grid_columns = mapping_determinant.shape[1]
    weight_rows = jnp.asarray(np.tile(weights, grid_rows // 4), jnp.float32)
    weight_columns = jnp.asarray(np.tile(weights, grid_columns // 4), jnp.float32)
    mass = mapping_determinant * weight_rows[:, None] * weight_columns[None, :]
    turns_rows = interface_rightangle_rotations[:, :, 0]
    turns_columns = interface_rightangle_rotations[:, :, 1]
    rotations = ((4 - jnp.roll(turns_rows, 1, axis=0)) % 4, turns_rows, (4 - jnp.roll(turns_columns, 1, axis=1)) % 4, turns_columns)
    flips = (jnp.roll(interface_flipped_markers[:, :, 0], 1, axis=0), interface_flipped_markers[:, :, 0], jnp.roll(interface_flipped_markers[:, :, 1], 1, axis=1), interface_flipped_markers[:, :, 1])
    valences = (jnp.roll(jnp.roll(corner_block_tally, 1, axis=0), 1, axis=1), jnp.roll(corner_block_tally, 1, axis=0), jnp.roll(corner_block_tally, 1, axis=1), corner_block_tally)
    mass_pieces = block_pieces(mass[None], N_FACE, N_TILE)

    def lone_layer(level_inputs):
        wind_pair, temp_level, thick_level, tracer_level, geo_level = level_inputs
        fields, courant, damping = advance(wind_pair[0], wind_pair[1], temp_level, thick_level, tracer_level, geo_level, inverse_mapping_entries, mapping_determinant, along_rows, along_columns)
        pieces = block_pieces(fields * mass, N_FACE, N_TILE)
        substep_outcome = combine_block(pieces, mass_pieces, rotations, flips, valences)
        field_count = substep_outcome.shape[0]
        return (substep_outcome.transpose(0, 1, 3, 2, 4).reshape(field_count, grid_rows, grid_columns), courant, damping)
    piled_layers, stepwise_advection_number_layerwise, hyperdiffusion_change_layerwise = lax.map(lone_layer, (jnp.moveaxis(airflow_components, 1, 0), heat_state, layer_pressure_depth, jnp.moveaxis(constituent_masses, 1, 0), gravity_potential_altitude))
    airflow_next = jnp.moveaxis(piled_layers[:, 0:2], 0, 1)
    heat_state_next = piled_layers[:, 2]
    pressure_depth_next = piled_layers[:, 3]
    constituent_masses_next = jnp.moveaxis(piled_layers[:, 4:], 0, 1)
    stepping_bounds = jnp.stack([jnp.max(stepwise_advection_number_layerwise), jnp.max(hyperdiffusion_change_layerwise)])
    return (airflow_next, heat_state_next, pressure_depth_next, constituent_masses_next, stepping_bounds)
```

```python
import math

import jax
import jax.numpy as jnp
import numpy as np
from jax import lax
from jax.experimental import pallas as pl
from jax.experimental.pallas import tpu as pltpu
from jax.sharding import Mesh
from jax.sharding import PartitionSpec as P

FACE = ("face_0", "face_1")
TILE = ("tile_0", "tile_1")
PLANE = ("face_1", "tile_0", "tile_1")

time_step = 0.05
viscosity = 0.05

PER_GROUP = 6
ROWS, LANES = 8, 128
VMEM = pl.BlockSpec(memory_space=pltpu.VMEM)
SMEM = pl.BlockSpec(memory_space=pltpu.SMEM)


def gll_tables():
    offset = 1.0 / math.sqrt(5.0)
    nodes = np.array([-1.0, -offset, offset, 1.0])
    weights = np.array([1.0 / 6.0, 5.0 / 6.0, 5.0 / 6.0, 1.0 / 6.0])
    bary = np.ones(4)
    for i in range(4):
        for j in range(4):
            if j != i:
                bary[i] = bary[i] / (nodes[i] - nodes[j])
    derivative = np.zeros((4, 4))
    for i in range(4):
        for j in range(4):
            if j != i:
                derivative[i, j] = bary[j] / bary[i] / (nodes[i] - nodes[j])
        derivative[i, i] = -np.sum(derivative[i])
    return derivative, weights


DERIVATIVE, WEIGHTS = gll_tables()


def iota(axis):
    return lax.broadcasted_iota(jnp.int32, (ROWS, LANES), axis)


def by_node(place, values):
    node = place % 4
    plane = jnp.full((ROWS, LANES), float(values[0]), jnp.float32)
    for i in range(1, 4):
        plane = jnp.where(node == i, float(values[i]), plane)
    return plane


def node_weights():
    return by_node(iota(0), WEIGHTS) * by_node(iota(1), WEIGHTS)


def derivative_terms(axis, scale):
    place = iota(axis)
    terms = []
    for k in range(-3, 4):
        values = [DERIVATIVE[i, i + k] if 0 <= i + k < 4 else 0.0 for i in range(4)]
        terms.append((k, by_node(place, values) * scale))
    return terms


def derive(field, axis, terms):
    size = field.shape[axis]
    total = None
    for k, coefficient in terms:
        moved = field if k == 0 else pltpu.roll(field, (-k) % size, axis)
        part = coefficient * moved
        total = part if total is None else total + part
    return total


def tile_of(index):
    return pl.ds(pl.multiple_of(index * ROWS, ROWS), ROWS)


def local_kernel(n_lev, air, heat, thick, tracer, ground, maps, det, w_out, left_out, right_out, share_out):
    levels = heat.shape[0]
    tracers = tracer.shape[0]
    fields = 4 + tracers
    groups = left_out.shape[0]
    lane = iota(1)
    ww = node_weights()
    j = det[...]
    mass = j * ww
    m00, m01, m10, m11 = maps[0], maps[1], maps[2], maps[3]
    j00, j01, j10, j11 = j * m00, j * m01, j * m10, j * m11
    scale = time_step * ww
    undo = 1.0 / scale
    b11 = (j00 * m00 + j01 * m01) * undo
    b12 = (j00 * m10 + j01 * m11) * undo
    b22 = (j10 * m10 + j11 * m11) * undo
    along_rows = derivative_terms(0, scale)
    along_columns = derivative_terms(1, scale)
    ground_plane = ground[...]

    def flux(first, second):
        return derive(first, 0, along_rows) + derive(second, 1, along_columns)

    def one(turn, carry):
        below, speed, damp, lefts, rights = carry
        lefts, rights = list(lefts), list(rights)
        level = levels - 1 - turn
        u, v = air[0, level], air[1, level]
        heat_l, thick_l = heat[level], thick[level]
        relative = lane - level

        def put(field, value):
            w_out[tile_of(field * levels + level), :] = value
            group = field // PER_GROUP
            here = relative == (field % PER_GROUP) * levels
            lefts[group] = jnp.where(here, value[:, 0:1], lefts[group])
            rights[group] = jnp.where(here, value[:, LANES - 1 : LANES], rights[group])

        term = heat_l * thick_l
        square = u * u + v * v
        energy = 0.5 * square + (ground_plane + below + 0.5 * term)
        below = below + term
        speed = jnp.maximum(speed, square)
        first, second = j00 * u + j01 * v, j10 * u + j11 * v

        rows, columns = derive(energy, 0, along_rows), derive(energy, 1, along_columns)
        put(0, mass * u - (j00 * rows + j10 * columns))
        put(1, mass * v - (j01 * rows + j11 * columns))
        rows, columns = derive(heat_l, 0, along_rows), derive(heat_l, 1, along_columns)
        put(2, mass * heat_l - (first * rows + second * columns))
        rows, columns = derive(thick_l, 0, along_rows), derive(thick_l, 1, along_columns)
        laplace = flux(b11 * rows + b12 * columns, b12 * rows + b22 * columns)
        damp = jnp.maximum(damp, jnp.abs(laplace))
        put(3, mass * thick_l - flux(thick_l * first, thick_l * second) + viscosity * laplace)
        for t in range(tracers):
            q = tracer[t, level]
            put(4 + t, mass * q - flux(q * first, q * second))
        return below, speed, damp, tuple(lefts), tuple(rights)

    zero = jnp.zeros((ROWS, LANES), jnp.float32)
    none = tuple(zero for _ in range(groups))
    total, speed, damp, lefts, rights = lax.fori_loop(0, levels, one, (zero, zero, zero, none, none))
    group, here = fields // PER_GROUP, lane == (fields % PER_GROUP) * levels
    lefts, rights = list(lefts), list(rights)
    lefts[group] = jnp.where(here, mass[:, 0:1], lefts[group])
    rights[group] = jnp.where(here, mass[:, LANES - 1 : LANES], rights[group])
    for g in range(groups):
        left_out[g] = lefts[g]
        right_out[g] = rights[g]
    w_out[pl.ds(fields * levels * ROWS, ROWS), :] = mass
    spare = w_out.shape[0] - (fields * levels + 1) * ROWS
    w_out[pl.ds((fields * levels + 1) * ROWS, spare), :] = jnp.zeros((spare, LANES), jnp.float32)
    spacing = jnp.sqrt(m00 * m00 + m01 * m01 + m10 * m10 + m11 * m11)
    courant = jnp.max(time_step * jnp.sqrt(speed) * spacing, axis=0, keepdims=True)
    damping = jnp.max(damp * (viscosity / mass), axis=0, keepdims=True)
    row = iota(0)
    bounds = jnp.where(row == 0, courant, damping)
    for peer in range(n_lev):
        share_out[peer, pl.ds(0, ROWS), :] = total
        share_out[peer, pl.ds(ROWS, ROWS), :] = bounds


def carry_kernel(levels, shared, w, lefts, rights, maps, det, wind_out, top_out, bottom_out, left_out, right_out, bound_out):
    me = lax.axis_index("lev")
    higher = jnp.zeros((ROWS, LANES), jnp.float32)
    bounds = shared[0, pl.ds(ROWS, ROWS), :]
    for peer in range(shared.shape[0]):
        higher = higher + jnp.where(peer > me, shared[peer, pl.ds(0, ROWS), :], 0.0)
        bounds = jnp.maximum(bounds, shared[peer, pl.ds(ROWS, ROWS), :])
    lane = iota(1)
    both = jnp.maximum(bounds, pltpu.roll(bounds, LANES // 2, 1))
    line = jnp.where(lane[0:1] < LANES // 2, both[0:1], both[1:2])
    bound_out[...] = jnp.broadcast_to(line[None], bound_out.shape)

    ww = node_weights()
    j = det[...]
    rows = derive(higher, 0, derivative_terms(0, time_step * ww))
    columns = derive(higher, 1, derivative_terms(1, time_step * ww))
    add_u = -j * (maps[0] * rows + maps[2] * columns)
    add_v = -j * (maps[1] * rows + maps[3] * columns)
    for field, add in ((0, add_u), (1, add_v)):
        for level in range(levels):
            at = pl.ds((field * levels + level) * ROWS, ROWS)
            wind_out[at, :] = w[at, :] + add
    is_u, is_v = lane < levels, (lane >= levels) & (lane < 2 * levels)

    def with_higher(ref, group, at):
        value = ref[group]
        if group == 0:
            value = value + jnp.where(is_u, add_u[:, at : at + 1], jnp.where(is_v, add_v[:, at : at + 1], 0.0))
        return value

    groups = lefts.shape[0]
    edge_rows = top_out.shape[0] - 2 * groups
    winds = 2 * levels
    for source, out, row in ((w, top_out, ROWS - 1), (w, bottom_out, 0)):
        for start in range(0, edge_rows, ROWS):
            out[pl.ds(start, ROWS), :] = source[pl.ds(start * ROWS + row, ROWS, stride=ROWS), :]
        out[pl.ds(0, levels), :] = out[pl.ds(0, levels), :] + add_u[row : row + 1]
        out[pl.ds(levels, levels), :] = out[pl.ds(levels, levels), :] + add_v[row : row + 1]
    for g in range(groups):
        left, right = with_higher(lefts, g, 0), with_higher(rights, g, LANES - 1)
        left_out[pl.ds(g * ROWS, ROWS), :] = left
        right_out[pl.ds(g * ROWS, ROWS), :] = right
        for out, row in ((top_out, ROWS - 1), (bottom_out, 0)):
            out[pl.ds(edge_rows + g, 1), :] = left[row : row + 1]
            out[pl.ds(edge_rows + groups + g, 1), :] = right[row : row + 1]


def turned(u, v, code):
    cosine = jnp.where(code == 0, 1.0, jnp.where(code == 2, -1.0, 0.0)).astype(jnp.float32)
    sine = jnp.where(code == 1, 1.0, jnp.where(code == 3, -1.0, 0.0)).astype(jnp.float32)
    return cosine * u - sine * v, sine * u + cosine * v


def sum_kernel(
    levels, n_face, n_tile, rotations, flips, valences, w, wind, up, down, west, east,
    air_out, heat_out, thick_out, tracer_out, up_rim, down_rim, west_rim, east_rim,
):
    face, tile = lax.axis_index(FACE), lax.axis_index(TILE)
    face_lower = lax.rem(face + n_face - 1, n_face)
    tile_lower = lax.rem(tile + n_tile - 1, n_tile)

    def at(f, t):
        return f * n_tile + t

    top_code = (4 - rotations[2 * at(face_lower, tile)]) & 3
    bottom_code = rotations[2 * at(face, tile)]
    west_code = (4 - rotations[2 * at(face, tile_lower) + 1]) & 3
    east_code = rotations[2 * at(face, tile) + 1]
    top_flip = flips[2 * at(face_lower, tile)]
    bottom_flip = flips[2 * at(face, tile)]
    west_flip = flips[2 * at(face, tile_lower) + 1]
    east_flip = flips[2 * at(face, tile) + 1]
    corners = {
        ("up", "west"): valences[at(face_lower, tile_lower)],
        ("up", "east"): valences[at(face_lower, tile)],
        ("down", "west"): valences[at(face, tile_lower)],
        ("down", "east"): valences[at(face, tile)],
    }
    row, lane = iota(0), iota(1)
    tracers = tracer_out.shape[0]
    fields = 4 + tracers
    groups = west_rim.shape[0]

    edge_rows = up_rim.shape[0]
    for source, out, flag in ((up, up_rim, top_flip), (down, down_rim, bottom_flip)):
        places = jnp.where(flag == 1, LANES - 1 - lane, lane)
        for start in range(0, edge_rows, ROWS):
            rows = pl.ds(start, ROWS)
            out[rows, :] = jnp.take_along_axis(source[rows, :], places, axis=1, mode="promise_in_bounds")

    def turn_packed(x, code):
        cosine = jnp.where(code == 0, 1.0, jnp.where(code == 2, -1.0, 0.0)).astype(jnp.float32)
        sine = jnp.where(code == 1, 1.0, jnp.where(code == 3, -1.0, 0.0)).astype(jnp.float32)
        later, earlier = pltpu.roll(x, LANES - levels, 1), pltpu.roll(x, levels, 1)
        out = cosine * x + sine * jnp.where(lane < levels, -later, earlier)
        return jnp.where(lane < 2 * levels, out, x)

    for source, out, flag, code, side in (
        (west, west_rim, west_flip, west_code, "west"),
        (east, east_rim, east_flip, east_code, "east"),
    ):
        for g in range(groups):
            x = source[pl.ds(g * ROWS, ROWS), :]
            backwards = jnp.concatenate(
                [source[pl.ds(g * ROWS + ROWS - 1 - r, 1), :] for r in range(ROWS)], axis=0
            )
            x = jnp.where(flag == 1, backwards, x)
            ends = []
            for end, row_code, start in (
                ("up", top_code, groups * ROWS),
                ("down", bottom_code, groups * ROWS + groups),
            ):
                corner = jnp.broadcast_to(source[pl.ds(start + g, 1), :], (ROWS, LANES))
                if g == 0:
                    corner = turn_packed(corner, (row_code + code) & 3)
                ends.append(jnp.where(corners[end, side] == 4, corner, 0.0))
            if g == 0:
                x = turn_packed(x, code)
            beside = jnp.where(row == 3, pltpu.roll(x, ROWS - 1, 0), jnp.where(row == 4, pltpu.roll(x, 1, 0), 0.0))
            beside = jnp.where(row == 0, ends[0], jnp.where(row == ROWS - 1, ends[1], beside))
            out[g] = x + beside

    first, last = lane == 0, lane == LANES - 1
    starts, stops = lane % 4 == 0, lane % 4 == 3

    def summed(x, upper, lower, west_column, east_column):
        beside = jnp.where(row == 3, pltpu.roll(x, ROWS - 1, 0), jnp.where(row == 4, pltpu.roll(x, 1, 0), 0.0))
        beside = jnp.where(row == 0, upper, jnp.where(row == ROWS - 1, lower, beside))
        x = x + beside
        beside = jnp.where(stops, pltpu.roll(x, LANES - 1, 1), jnp.where(starts, pltpu.roll(x, 1, 1), 0.0))
        beside = jnp.where(first, west_column, jnp.where(last, east_column, beside))
        return x + beside

    def rim(ref, index):
        return jnp.broadcast_to(ref[pl.ds(index, 1), :], (ROWS, LANES))

    def columns(packed, slot, place):
        return pltpu.roll(packed, (place - slot) % LANES, 1)

    index = fields * levels
    group, slot = fields // PER_GROUP, (fields % PER_GROUP) * levels
    mass = summed(
        w[pl.ds(index * ROWS, ROWS), :], rim(up_rim, index), rim(down_rim, index),
        columns(west_rim[group], slot, 0), columns(east_rim[group], slot, LANES - 1),
    )
    scale = 1.0 / mass

    def one(level, _):
        shift = lax.rem(LANES - level, LANES)
        wests = [pltpu.roll(west_rim[g], shift, 1) for g in range(groups)]
        easts = [pltpu.roll(east_rim[g], shift, 1) for g in range(groups)]

        def out(field, x, upper, lower):
            group, slot = field // PER_GROUP, (field % PER_GROUP) * levels
            sums = summed(x, upper, lower, columns(wests[group], slot, 0), columns(easts[group], slot, LANES - 1))
            return sums * scale

        u_at, v_at = level, levels + level
        upper = turned(rim(up_rim, u_at), rim(up_rim, v_at), top_code)
        lower = turned(rim(down_rim, u_at), rim(down_rim, v_at), bottom_code)
        air_out[0, level] = out(0, wind[tile_of(u_at), :], upper[0], lower[0])
        air_out[1, level] = out(1, wind[tile_of(v_at), :], upper[1], lower[1])

        def plain(field):
            index = field * levels + level
            return out(field, w[tile_of(index), :], rim(up_rim, index), rim(down_rim, index))

        heat_out[level] = plain(2)
        thick_out[level] = plain(3)
        for t in range(tracers):
            tracer_out[t, level] = plain(4 + t)
        return 0

    lax.fori_loop(0, levels, one, 0)


def shift(x, axes, step):
    count = lax.axis_size(axes)
    return lax.ppermute(x, axes, [(i, (i + step) % count) for i in range(count)])


def on_device(air, heat, thick, tracer, ground, maps, det, rotations, flips, valences):
    levels = heat.shape[0]
    tracers = tracer.shape[0]
    fields = 4 + tracers
    tiles = fields * levels + 1
    edge_rows = -(-tiles // ROWS) * ROWS
    groups = fields // PER_GROUP + 1
    n_lev = lax.axis_size("lev")
    n_face, n_tile = lax.axis_size(FACE), lax.axis_size(TILE)
    n_plane = lax.axis_size(PLANE)

    def f32(*shape):
        return jax.ShapeDtypeStruct(shape, jnp.float32)

    params = pltpu.CompilerParams(vmem_limit_bytes=24 * 1024 * 1024)
    w, lefts, rights, share = pl.pallas_call(
        lambda *refs: local_kernel(n_lev, *refs),
        out_shape=(f32(edge_rows * ROWS, LANES), f32(groups, ROWS, LANES), f32(groups, ROWS, LANES), f32(n_lev, 2 * ROWS, LANES)),
        in_specs=[VMEM] * 7,
        out_specs=(VMEM,) * 4,
        compiler_params=params,
        name="local",
    )(air, heat, thick, tracer, ground, maps, det)
    shared = lax.all_to_all(share, "lev", 0, 0, tiled=True)
    wind, top, bottom, left, right, bound = pl.pallas_call(
        lambda *refs: carry_kernel(levels, *refs),
        out_shape=(
            f32(2 * levels * ROWS, LANES),
            f32(edge_rows + 2 * groups, LANES),
            f32(edge_rows + 2 * groups, LANES),
            f32(groups * ROWS, LANES),
            f32(groups * ROWS, LANES),
            f32(n_plane, 1, LANES),
        ),
        in_specs=[VMEM] * 6,
        out_specs=(VMEM,) * 6,
        compiler_params=params,
        name="carry",
    )(shared, w, lefts, rights, maps, det)
    up = shift(top, FACE, 1)
    down = shift(bottom, FACE, -1)
    plane = lax.all_to_all(bound, PLANE, 0, 0, tiled=True)
    bounds = lax.pmax(jnp.max(plane[:, 0, :], axis=0), "face_0")
    stepping_bounds = jnp.max(bounds.reshape(2, LANES // 2), axis=1)
    ends = edge_rows + groups
    to_east = jnp.concatenate([right, up[ends:], down[ends:]], 0)
    to_west = jnp.concatenate([left, up[edge_rows:ends], down[edge_rows:ends]], 0)
    west = shift(to_east, TILE, 1)
    east = shift(to_west, TILE, -1)
    air_next, heat_next, thick_next, tracer_next = pl.pallas_call(
        lambda *refs: sum_kernel(levels, n_face, n_tile, *refs),
        out_shape=(f32(*air.shape), f32(*heat.shape), f32(*thick.shape), f32(*tracer.shape)),
        in_specs=[SMEM] * 3 + [VMEM] * 6,
        out_specs=(VMEM,) * 4,
        scratch_shapes=[
            pltpu.VMEM((edge_rows, LANES), jnp.float32),
            pltpu.VMEM((edge_rows, LANES), jnp.float32),
            pltpu.VMEM((groups, ROWS, LANES), jnp.float32),
            pltpu.VMEM((groups, ROWS, LANES), jnp.float32),
        ],
        compiler_params=params,
        name="sum",
    )(rotations.reshape(-1), flips.reshape(-1), valences.reshape(-1), w, wind, up, down, west, east)
    return air_next, heat_next, thick_next, tracer_next, stepping_bounds


def solution(mesh):
    face, tile, lev = mesh.shape["face"], mesh.shape["tile"], mesh.shape["lev"]
    inner = min(face, 4)
    split = Mesh(
        mesh.devices.reshape(face // inner, inner, tile // 2, 2, lev),
        ("face_0", "face_1", "tile_0", "tile_1", "lev"),
    )
    level_plane = P("lev", FACE, TILE)
    field_level_plane = P(None, "lev", FACE, TILE)
    return jax.shard_map(
        on_device,
        mesh=split,
        in_specs=(
            field_level_plane, level_plane, level_plane, field_level_plane,
            P(FACE, TILE), P(None, FACE, TILE), P(FACE, TILE), P(), P(), P(),
        ),
        out_specs=(field_level_plane, level_plane, level_plane, field_level_plane, P()),
        check_vma=False,
    )
```

```python
import math

import jax
import jax.numpy as jnp
import numpy as np
from jax import lax
from jax.experimental import pallas as pl
from jax.experimental.pallas import tpu as pltpu
from jax.sharding import Mesh
from jax.sharding import PartitionSpec as P


FACE = ("face_0", "face_1")
TILE = ("tile_0", "tile_1")
PLANE = FACE + ("tile_0",)
COLUMN = ("tile_1", "lev")

time_step = 0.05
viscosity = 0.05

ROWS, LANES = 8, 128
VMEM = pl.BlockSpec(memory_space=pltpu.VMEM)
ANY = pl.BlockSpec(memory_space=pltpu.HBM)
SMEM = pl.BlockSpec(memory_space=pltpu.SMEM)


def gll_tables():
    offset = 1.0 / math.sqrt(5.0)
    nodes = np.array([-1.0, -offset, offset, 1.0])
    weights = np.array([1.0 / 6.0, 5.0 / 6.0, 5.0 / 6.0, 1.0 / 6.0])
    bary = np.ones(4)
    for i in range(4):
        for j in range(4):
            if j != i:
                bary[i] = bary[i] / (nodes[i] - nodes[j])
    derivative = np.zeros((4, 4))
    for i in range(4):
        for j in range(4):
            if j != i:
                derivative[i, j] = bary[j] / bary[i] / (nodes[i] - nodes[j])
        derivative[i, i] = -np.sum(derivative[i])
    return derivative, weights


DERIVATIVE, WEIGHTS = gll_tables()


def iota(axis):
    return lax.broadcasted_iota(jnp.int32, (ROWS, LANES), axis)


def by_node(place, values):
    node = place % 4
    plane = jnp.full((ROWS, LANES), float(values[0]), jnp.float32)
    for i in range(1, 4):
        plane = jnp.where(node == i, float(values[i]), plane)
    return plane


def node_weights():
    return by_node(iota(0), WEIGHTS) * by_node(iota(1), WEIGHTS)


def derivative_terms(axis, scale):
    place = iota(axis)
    terms = []
    for k in range(-3, 4):
        values = [DERIVATIVE[i, i + k] if 0 <= i + k < 4 else 0.0 for i in range(4)]
        terms.append((k, by_node(place, values) * scale))
    return terms


def derive(field, axis, terms):
    size = field.shape[axis]
    total = None
    for k, coefficient in terms:
        moved = field if k == 0 else pltpu.roll(field, (-k) % size, axis)
        part = coefficient * moved
        total = part if total is None else total + part
    return total


def tile_of(index):
    return pl.ds(pl.multiple_of(index * ROWS, ROWS), ROWS)


def beside_in_block(x, axis):
    place, size = iota(axis), x.shape[axis]
    later, earlier = pltpu.roll(x, size - 1, axis), pltpu.roll(x, 1, axis)
    before_border = (place % 4 == 3) & (place < size - 1)
    after_border = (place % 4 == 0) & (place > 0)
    return jnp.where(before_border, later, jnp.where(after_border, earlier, 0.0))


def sum_in_block(x):
    x = x + beside_in_block(x, 1)
    return x + beside_in_block(x, 0)


def lane_tables():
    swap = np.zeros((LANES, LANES))
    for c in range(3, LANES - 1, 4):
        swap[c, c + 1] = swap[c + 1, c] = 1.0
    derive_columns = np.kron(np.eye(LANES // 4), (WEIGHTS[:, None] * DERIVATIVE).T)
    full = -(derive_columns @ (np.eye(LANES) + swap)).astype(np.float32)
    high = full.astype(jnp.bfloat16)
    low = (full - high.astype(np.float32)).astype(jnp.bfloat16)
    swap = swap.astype(jnp.bfloat16)
    return np.concatenate([swap, swap, high, high, low], 0)


def halves(x):
    high = x.astype(jnp.bfloat16)
    return high, (x - high.astype(jnp.float32)).astype(jnp.bfloat16)


def pair_of(lane):
    return ((lane + 1) // 2) % (LANES // 2)


def local_kernel(
    n_share, air_in, heat_in, thick_in, tracer_in, ground_in, maps_in, det_in, table_in, w_out, packed_out, share_out,
    air, heat, thick, tracer, ground, maps, det, table, small_sem, tracer_sem,
):
    levels = heat.shape[0]
    small = [
        pltpu.make_async_copy(source, held, small_sem.at[i])
        for i, (source, held) in enumerate(
            (
                (maps_in, maps), (det_in, det), (ground_in, ground), (heat_in, heat), (thick_in, thick),
                (air_in, air), (table_in, table),
            )
        )
    ]

    def tracer_copy(level):
        return pltpu.make_async_copy(tracer_in.at[:, level], tracer.at[:, level], tracer_sem.at[level])

    for copy in small:
        copy.start()
    for level in reversed(range(levels)):
        tracer_copy(level).start()
    for copy in small:
        copy.wait()
    tracers = tracer.shape[0]
    fields = 4 + tracers
    row, lane = iota(0), iota(1)
    pair = pair_of(lane)
    row_scale = time_step * by_node(row, WEIGHTS)
    j = det[...]
    mass = j * node_weights()
    m00, m01, m10, m11 = maps[0], maps[1], maps[2], maps[3]
    j00, j01, j10, j11 = j * m00, j * m01, j * m10, j * m11
    scale = time_step * node_weights()
    undo = 1.0 / scale
    b11 = (j00 * m00 + j01 * m01) * undo
    b12 = (j00 * m10 + j01 * m11) * undo
    b22 = (j10 * m10 + j11 * m11) * undo
    along_rows = derivative_terms(0, scale)
    along_columns = derivative_terms(1, scale)
    ground_plane = ground[...]

    def one_level(level, below, speed, damp):
        u, v = air[0, level], air[1, level]
        heat_l, thick_l = heat[level], thick[level]
        term = heat_l * thick_l
        square = u * u + v * v
        energy = 0.5 * square + (ground_plane + below + 0.5 * term)
        below = below + term
        speed = jnp.maximum(speed, square)
        first, second = j00 * u + j01 * v, j10 * u + j11 * v
        second_scaled = second * row_scale

        rows, columns = derive(energy, 0, along_rows), derive(energy, 1, along_columns)
        plain = [mass * u - (j00 * rows + j10 * columns), mass * v - (j01 * rows + j11 * columns)]
        rows, columns = derive(heat_l, 0, along_rows), derive(heat_l, 1, along_columns)
        plain.append(mass * heat_l - (first * rows + second * columns))
        rows, columns = derive(thick_l, 0, along_rows), derive(thick_l, 1, along_columns)
        laplace = derive(b11 * rows + b12 * columns, 0, along_rows) + derive(b12 * rows + b22 * columns, 1, along_columns)
        damp = jnp.maximum(damp, jnp.abs(laplace))
        plain.append(mass * thick_l - derive(thick_l * first, 0, along_rows) + viscosity * laplace)
        fluxes = [thick_l * second_scaled]
        tracer_copy(level).wait()
        for t in range(tracers):
            q = tracer[t, level]
            plain.append(mass * q - derive(q * first, 0, along_rows))
            fluxes.append(q * second_scaled)
        fluxes.append(jnp.zeros_like(u))
        return below, speed, damp, plain, fluxes

    def through(plain, fluxes):
        high, low = halves(jnp.concatenate(plain, axis=0))
        swapped = jnp.dot(
            jnp.concatenate([high, low], axis=1), table[pl.ds(0, 2 * LANES), :], preferred_element_type=jnp.float32
        )
        high, low = halves(jnp.concatenate(fluxes, axis=0))
        derived = jnp.dot(
            jnp.concatenate([high, low, high], axis=1), table[pl.ds(2 * LANES, 3 * LANES), :],
            preferred_element_type=jnp.float32,
        )
        return swapped, derived

    def finish_level(level, slot, plain, swapped, derived, packed):
        for field in range(fields):
            x = plain[field] + swapped[field * ROWS : field * ROWS + ROWS]
            if field >= 3:
                x = x + derived[(field - 3) * ROWS : (field - 3) * ROWS + ROWS]
            x = x + beside_in_block(x, 0)
            w_out[tile_of(field * levels + level), :] = x
            packed = jnp.where(pair == slot + field, pltpu.roll(x, 2 * (slot + field), 1), packed)
        return packed

    summed_mass = sum_in_block(mass)
    packed_mass = pltpu.roll(summed_mass, 4 * fields, 1)

    def one(turn, carry):
        below, speed, damp = carry
        half = levels // 2 - 1 - turn
        packed = jnp.where(pair == 2 * fields, packed_mass, 0.0)
        below, speed, damp, plain_1, fluxes_1 = one_level(2 * half + 1, below, speed, damp)
        below, speed, damp, plain_0, fluxes_0 = one_level(2 * half, below, speed, damp)
        swapped, derived = through(plain_1 + plain_0, fluxes_1 + fluxes_0)
        n, m = len(plain_1) * ROWS, len(fluxes_1) * ROWS
        packed = finish_level(2 * half + 1, fields, plain_1, swapped[:n], derived[:m], packed)
        packed = finish_level(2 * half, 0, plain_0, swapped[n:], derived[m:], packed)
        packed_out[tile_of(half), :] = packed
        return below, speed, damp

    zero = jnp.zeros((ROWS, LANES), jnp.float32)
    total, speed, damp = lax.fori_loop(0, levels // 2, one, (zero, zero, zero), unroll=3)
    w_out[pl.ds(fields * levels * ROWS, ROWS), :] = summed_mass
    spare = w_out.shape[0] - (fields * levels + 1) * ROWS
    w_out[pl.ds((fields * levels + 1) * ROWS, spare), :] = jnp.zeros((spare, LANES), jnp.float32)
    spacing = jnp.sqrt(m00 * m00 + m01 * m01 + m10 * m10 + m11 * m11)
    courant = jnp.max(time_step * jnp.sqrt(speed) * spacing, axis=0, keepdims=True)
    damping = jnp.max(damp * (viscosity / mass), axis=0, keepdims=True)
    bounds = jnp.where(row == 0, courant, damping)
    for peer in range(n_share):
        share_out[peer, pl.ds(0, ROWS), :] = total
        share_out[peer, pl.ds(ROWS, ROWS), :] = bounds


def carry_kernel(levels, n_lev, shared, w, packed, maps, det, wind_out, far_out, near_out, packed_out, bound_out):
    lev, core = lax.axis_index("lev"), lax.axis_index("tile_1")
    odd = lax.rem(lax.axis_index(FACE), 2) == 1
    higher = jnp.zeros((ROWS, LANES), jnp.float32)
    bounds = shared[0, pl.ds(ROWS, ROWS), :]
    for peer in range(shared.shape[0]):
        counts = (peer // n_lev == core) & (peer % n_lev > lev)
        higher = higher + jnp.where(counts, shared[peer, pl.ds(0, ROWS), :], 0.0)
        bounds = jnp.maximum(bounds, shared[peer, pl.ds(ROWS, ROWS), :])
    lane = iota(1)
    pair = pair_of(lane)
    both = jnp.maximum(bounds, pltpu.roll(bounds, LANES // 2, 1))
    line = jnp.where(lane[0:1] < LANES // 2, both[0:1], both[1:2])
    bound_out[...] = jnp.broadcast_to(line[None], bound_out.shape)

    scale = time_step * node_weights()
    j = det[...]
    rows = derive(higher, 0, derivative_terms(0, scale))
    columns = derive(higher, 1, derivative_terms(1, scale))
    add_u = sum_in_block(-j * (maps[0] * rows + maps[2] * columns))
    add_v = sum_in_block(-j * (maps[1] * rows + maps[3] * columns))
    for field, add in ((0, add_u), (1, add_v)):
        for level in range(levels):
            at = pl.ds((field * levels + level) * ROWS, ROWS)
            wind_out[at, :] = w[at, :] + add
    halves_of_levels = packed.shape[0] // ROWS
    corner_rows = 2 * ROWS
    edge_rows = far_out.shape[0] - corner_rows
    for start in range(0, edge_rows, ROWS):
        last = w[pl.ds(start * ROWS + ROWS - 1, ROWS, stride=ROWS), :]
        first = w[pl.ds(start * ROWS, ROWS, stride=ROWS), :]
        far_out[pl.ds(start, ROWS), :] = jnp.where(odd, last, first)
        near_out[pl.ds(start, ROWS), :] = jnp.where(odd, first, last)
    for out, ends in ((far_out, odd), (near_out, jnp.logical_not(odd))):
        for start, add in ((0, add_u), (levels, add_v)):
            at = pl.ds(start, levels)
            out[at, :] = out[at, :] + jnp.where(ends, add[ROWS - 1 : ROWS], add[0:1])
        out[pl.ds(edge_rows, corner_rows), :] = jnp.zeros((corner_rows, LANES), jnp.float32)
    n_fields = (w.shape[0] // ROWS - 1) // levels
    add = jnp.zeros((ROWS, LANES), jnp.float32)
    for slot in (0, n_fields):
        add = jnp.where(pair == slot, pltpu.roll(add_u, 2 * slot, 1), add)
        add = jnp.where(pair == slot + 1, pltpu.roll(add_v, 2 * slot + 2, 1), add)
    for half in range(halves_of_levels):
        at = pl.ds(half * ROWS, ROWS)
        x = packed[at, :] + add
        packed_out[at, :] = x
        for out, ends in ((far_out, odd), (near_out, jnp.logical_not(odd))):
            out[pl.ds(edge_rows + half, 1), :] = jnp.where(ends, x[ROWS - 1 : ROWS], x[0:1])


def cosine_sine(code):
    cosine = jnp.where(code == 0, 1.0, jnp.where(code == 2, -1.0, 0.0)).astype(jnp.float32)
    sine = jnp.where(code == 1, 1.0, jnp.where(code == 3, -1.0, 0.0)).astype(jnp.float32)
    return cosine, sine


def turned(u, v, code):
    cosine, sine = cosine_sine(code)
    return cosine * u - sine * v, sine * u + cosine * v


def sum_kernel(
    levels, n_face, n_tile, rotations, flips, valences, w, wind, far, near, inside, outside,
    air_out, heat_out, thick_out, tracer_out, up_rim, down_rim, side_rim,
    air_held, heat_held, thick_held, tracer_held, out_sem,
):
    face, tile = lax.axis_index(FACE), lax.axis_index(TILE)
    face_lower = lax.rem(face + n_face - 1, n_face)
    tile_lower = lax.rem(tile + n_tile - 1, n_tile)

    def at(f, t):
        return f * n_tile + t

    top_code = (4 - rotations[2 * at(face_lower, tile)]) & 3
    bottom_code = rotations[2 * at(face, tile)]
    west_code = (4 - rotations[2 * at(face, tile_lower) + 1]) & 3
    east_code = rotations[2 * at(face, tile) + 1]
    top_flip = flips[2 * at(face_lower, tile)]
    bottom_flip = flips[2 * at(face, tile)]
    west_flip = flips[2 * at(face, tile_lower) + 1]
    east_flip = flips[2 * at(face, tile) + 1]
    corners = {
        ("up", "west"): valences[at(face_lower, tile_lower)],
        ("up", "east"): valences[at(face_lower, tile)],
        ("down", "west"): valences[at(face, tile_lower)],
        ("down", "east"): valences[at(face, tile)],
    }
    row, lane = iota(0), iota(1)
    pair = pair_of(lane)
    tracers = tracer_out.shape[0]
    fields = 4 + tracers
    count = side_rim.shape[0]

    edge_rows = up_rim.shape[0]
    odd_face, odd_tile = lax.rem(face, 2) == 1, lax.rem(tile, 2) == 1
    for out, flag, by_near in ((up_rim, top_flip, odd_face), (down_rim, bottom_flip, jnp.logical_not(odd_face))):
        places = jnp.where(flag == 1, LANES - 1 - lane, lane)
        for start in range(0, edge_rows, ROWS):
            rows = pl.ds(start, ROWS)
            x = jnp.where(by_near, near[rows, :], far[rows, :])
            out[rows, :] = jnp.take_along_axis(x, places, axis=1, mode="promise_in_bounds")

    within = jnp.where(pair >= fields, pair - fields, pair)
    is_u, is_v = (within == 0) & (pair < 2 * fields), within == 1

    def turn_packed(x, code):
        cosine, sine = cosine_sine(code)
        rows = x.shape[0]
        u, v = (jnp.broadcast_to(mask[0:1], (rows, LANES)) for mask in (is_u.astype(jnp.int32), is_v.astype(jnp.int32)))
        from_v, from_u = pltpu.roll(x, LANES - 2, 1), pltpu.roll(x, 2, 1)
        return jnp.where(u == 1, cosine * x - sine * from_v, jnp.where(v == 1, sine * from_u + cosine * x, x))

    def side(from_inside, flag, code, name):
        def rows_at(start, rows):
            at = pl.ds(start, rows)
            return jnp.where(from_inside, inside[at, :], outside[at, :])

        far_end, near_end = rows_at(count * ROWS, 2 * ROWS), rows_at((count + 2) * ROWS, 2 * ROWS)
        ends = []
        for end, row_code, by_near in (("up", top_code, odd_face), ("down", bottom_code, jnp.logical_not(odd_face))):
            corner = turn_packed(jnp.where(by_near, near_end, far_end), (row_code + code) & 3)
            ends.append(jnp.where(corners[end, name] == 4, corner, 0.0))
        columns = []
        for half in range(count):
            start = half * ROWS
            x = jnp.concatenate(
                [rows_at(start + jnp.where(flag == 1, ROWS - 1 - r, r), 1) for r in range(ROWS)], axis=0
            )
            x = turn_packed(x, code)
            over = [jnp.broadcast_to(end[half : half + 1], (ROWS, LANES)) for end in ends]
            columns.append(x + jnp.where(row == 0, over[0], jnp.where(row == ROWS - 1, over[1], 0.0)))
        return columns

    wests = side(odd_tile, west_flip, west_code, "west")
    easts = side(jnp.logical_not(odd_tile), east_flip, east_code, "east")
    for half in range(count):
        side_rim[half] = jnp.where(lane % 2 == 0, pltpu.roll(wests[half], 1, 1), pltpu.roll(easts[half], LANES - 1, 1))

    at_side = (lane == 0) | (lane == LANES - 1)

    def summed(x, upper, lower, sides, slot):
        x = x + jnp.where(row == 0, upper, jnp.where(row == ROWS - 1, lower, 0.0))
        moved = pltpu.roll(sides, (LANES - 2 * slot) % LANES, 1) if slot else sides
        return x + jnp.where(at_side, moved, 0.0)

    def rim(ref, index):
        return jnp.broadcast_to(ref[pl.ds(index, 1), :], (ROWS, LANES))

    index = fields * levels
    mass = summed(w[pl.ds(index * ROWS, ROWS), :], rim(up_rim, index), rim(down_rim, index), side_rim[0], 2 * fields)
    scale = 1.0 / mass

    def one(half, _):
        sides = side_rim[half]
        for part in range(2):
            level, slot = 2 * half + part, part * fields
            u_at, v_at = level, levels + level
            upper = turned(rim(up_rim, u_at), rim(up_rim, v_at), top_code)
            lower = turned(rim(down_rim, u_at), rim(down_rim, v_at), bottom_code)
            air_held[0, level] = summed(wind[tile_of(u_at), :], upper[0], lower[0], sides, slot) * scale
            air_held[1, level] = summed(wind[tile_of(v_at), :], upper[1], lower[1], sides, slot + 1) * scale
            for field in range(2, fields):
                index = field * levels + level
                x = w[tile_of(index), :]
                x = summed(x, rim(up_rim, index), rim(down_rim, index), sides, slot + field) * scale
                if field == 2:
                    heat_held[level] = x
                elif field == 3:
                    thick_held[level] = x
                else:
                    tracer_held[field - 4, level] = x
            for copy in copies_out(level):
                copy.start()
        return 0

    def copies_out(level):
        return (
            pltpu.make_async_copy(air_held.at[:, level], air_out.at[:, level], out_sem.at[0, level]),
            pltpu.make_async_copy(heat_held.at[level], heat_out.at[level], out_sem.at[1, level]),
            pltpu.make_async_copy(thick_held.at[level], thick_out.at[level], out_sem.at[2, level]),
            pltpu.make_async_copy(tracer_held.at[:, level], tracer_out.at[:, level], out_sem.at[3, level]),
        )

    def finish(level, _):
        for copy in copies_out(level):
            copy.wait()
        return 0

    lax.fori_loop(0, levels // 2, one, 0)
    lax.fori_loop(0, levels, finish, 0)


def swap_pairs(x, axes, start):
    count = lax.axis_size(axes)
    pairs = [(i % count, (i + 1) % count) for i in range(start, count + start, 2)]
    return lax.ppermute(x, axes, pairs + [(j, i) for i, j in pairs])


def bounds_kernel(plane, out):
    both = jnp.max(plane[...], axis=0)
    lane = lax.broadcasted_iota(jnp.int32, (1, LANES), 1)
    for i in range(2):
        out[i] = jnp.max(jnp.where(lane // (LANES // 2) == i, both, 0.0))


def on_device(air, heat, thick, tracer, ground, maps, det, rotations, flips, valences):
    levels = heat.shape[0]
    tracers = tracer.shape[0]
    fields = 4 + tracers
    edge_rows = -(-(fields * levels + 1) // ROWS) * ROWS
    count = levels // 2
    n_lev = lax.axis_size("lev")
    n_share = lax.axis_size(COLUMN)
    n_face, n_tile = lax.axis_size(FACE), lax.axis_size(TILE)
    n_plane = lax.axis_size(PLANE)

    def f32(*shape):
        return jax.ShapeDtypeStruct(shape, jnp.float32)

    inputs = (air, heat, thick, tracer, ground, maps, det, jnp.asarray(lane_tables()))
    inputs = tuple(pltpu.with_memory_space_constraint(x, pltpu.HBM) for x in inputs)
    params = pltpu.CompilerParams(vmem_limit_bytes=24 * 1024 * 1024)
    w, packed, share = pl.pallas_call(
        lambda *refs: local_kernel(n_share, *refs),
        out_shape=(f32(edge_rows * ROWS, LANES), f32(count * ROWS, LANES), f32(n_share, 2 * ROWS, LANES)),
        in_specs=[ANY] * 8,
        out_specs=(VMEM,) * 3,
        scratch_shapes=[pltpu.VMEM(x.shape, x.dtype) for x in inputs]
        + [pltpu.SemaphoreType.DMA((7,)), pltpu.SemaphoreType.DMA((levels,))],
        compiler_params=params,
        name="local",
    )(*inputs)
    shared = lax.all_to_all(share, COLUMN, 0, 0, tiled=True)
    wind, far, near, packed, bound = pl.pallas_call(
        lambda *refs: carry_kernel(levels, n_lev, *refs),
        out_shape=(
            f32(2 * levels * ROWS, LANES),
            f32(edge_rows + 2 * ROWS, LANES),
            f32(edge_rows + 2 * ROWS, LANES),
            f32(count * ROWS, LANES),
            f32(n_plane, 1, LANES),
        ),
        in_specs=[VMEM] * 5,
        out_specs=(VMEM,) * 5,
        compiler_params=params,
        name="carry",
    )(shared, w, packed, maps, det)
    far = swap_pairs(far, FACE, 1)
    near = swap_pairs(near, FACE, 0)
    plane = lax.all_to_all(bound, PLANE, 0, 0, tiled=True)
    stepping_bounds = pl.pallas_call(
        bounds_kernel, out_shape=f32(2), in_specs=[VMEM], out_specs=SMEM, compiler_params=params, name="bounds"
    )(plane)
    sides = jnp.concatenate([packed, far[edge_rows:], near[edge_rows:]], 0)
    inside = swap_pairs(sides, TILE, 0)
    outside = swap_pairs(sides, TILE, 1)
    sums = pl.pallas_call(
        lambda *refs: sum_kernel(levels, n_face, n_tile, *refs),
        out_shape=(f32(*air.shape), f32(*heat.shape), f32(*thick.shape), f32(*tracer.shape)),
        in_specs=[SMEM] * 3 + [VMEM] * 6,
        out_specs=(ANY,) * 4,
        scratch_shapes=[
            pltpu.VMEM((edge_rows, LANES), jnp.float32),
            pltpu.VMEM((edge_rows, LANES), jnp.float32),
            pltpu.VMEM((count, ROWS, LANES), jnp.float32),
            *(pltpu.VMEM(x.shape, jnp.float32) for x in (air, heat, thick, tracer)),
            pltpu.SemaphoreType.DMA((4, levels)),
        ],
        compiler_params=params,
        name="sum",
    )
    air_next, heat_next, thick_next, tracer_next = sums(rotations.reshape(-1), flips.reshape(-1), valences.reshape(-1), w, wind, far, near, inside, outside)
    return air_next, heat_next, thick_next, tracer_next, stepping_bounds


def solution(mesh):
    face, tile, lev = mesh.shape["face"], mesh.shape["tile"], mesh.shape["lev"]
    inner = min(face, 4)
    split = Mesh(
        mesh.devices.reshape(face // inner, inner, tile // 2, 2, lev),
        ("face_0", "face_1", "tile_0", "tile_1", "lev"),
    )
    level_plane = P("lev", FACE, TILE)
    field_level_plane = P(None, "lev", FACE, TILE)
    return jax.shard_map(
        on_device,
        mesh=split,
        in_specs=(
            field_level_plane, level_plane, level_plane, field_level_plane,
            P(FACE, TILE), P(None, FACE, TILE), P(FACE, TILE), P(), P(), P(),
        ),
        out_specs=(field_level_plane, level_plane, level_plane, field_level_plane, P()),
        check_vma=False,
    )
```

```python
import math

import jax
import jax.numpy as jnp
import numpy as np
from jax import lax
from jax.experimental import pallas as pl
from jax.experimental.pallas import tpu as pltpu
from jax.sharding import Mesh
from jax.sharding import PartitionSpec as P


FACE = ("face_0", "face_1")
TILE = ("tile_0", "tile_1")
PLANE = FACE + ("tile_0",)
COLUMN = ("tile_1", "lev")

time_step = 0.05
viscosity = 0.05

ROWS, LANES = 8, 128
VMEM = pl.BlockSpec(memory_space=pltpu.VMEM)
ANY = pl.BlockSpec(memory_space=pltpu.HBM)
SMEM = pl.BlockSpec(memory_space=pltpu.SMEM)


def gll_tables():
    offset = 1.0 / math.sqrt(5.0)
    nodes = np.array([-1.0, -offset, offset, 1.0])
    weights = np.array([1.0 / 6.0, 5.0 / 6.0, 5.0 / 6.0, 1.0 / 6.0])
    bary = np.ones(4)
    for i in range(4):
        for j in range(4):
            if j != i:
                bary[i] = bary[i] / (nodes[i] - nodes[j])
    derivative = np.zeros((4, 4))
    for i in range(4):
        for j in range(4):
            if j != i:
                derivative[i, j] = bary[j] / bary[i] / (nodes[i] - nodes[j])
        derivative[i, i] = -np.sum(derivative[i])
    return derivative, weights


DERIVATIVE, WEIGHTS = gll_tables()


def iota(axis):
    return lax.broadcasted_iota(jnp.int32, (ROWS, LANES), axis)


def by_node(place, values):
    node = place % 4
    plane = jnp.full((ROWS, LANES), float(values[0]), jnp.float32)
    for i in range(1, 4):
        plane = jnp.where(node == i, float(values[i]), plane)
    return plane


def node_weights():
    return by_node(iota(0), WEIGHTS) * by_node(iota(1), WEIGHTS)


def derivative_terms(axis, scale):
    place = iota(axis)
    terms = []
    for k in range(-3, 4):
        values = [DERIVATIVE[i, i + k] if 0 <= i + k < 4 else 0.0 for i in range(4)]
        terms.append((k, by_node(place, values) * scale))
    return terms


def derive(field, axis, terms):
    size = field.shape[axis]
    total = None
    for k, coefficient in terms:
        moved = field if k == 0 else pltpu.roll(field, (-k) % size, axis)
        part = coefficient * moved
        total = part if total is None else total + part
    return total


def tile_of(index):
    return pl.ds(pl.multiple_of(index * ROWS, ROWS), ROWS)


def beside_in_block(x, axis):
    place, size = iota(axis), x.shape[axis]
    later, earlier = pltpu.roll(x, size - 1, axis), pltpu.roll(x, 1, axis)
    before_border = (place % 4 == 3) & (place < size - 1)
    after_border = (place % 4 == 0) & (place > 0)
    return jnp.where(before_border, later, jnp.where(after_border, earlier, 0.0))


def sum_in_block(x):
    x = x + beside_in_block(x, 1)
    return x + beside_in_block(x, 0)


def lane_tables():
    swap = np.zeros((LANES, LANES))
    for c in range(3, LANES - 1, 4):
        swap[c, c + 1] = swap[c + 1, c] = 1.0
    derive_columns = np.kron(np.eye(LANES // 4), (WEIGHTS[:, None] * DERIVATIVE).T)
    full = -(derive_columns @ (np.eye(LANES) + swap)).astype(np.float32)
    high = full.astype(jnp.bfloat16)
    low = (full - high.astype(np.float32)).astype(jnp.bfloat16)
    swap = swap.astype(jnp.bfloat16)
    return np.concatenate([swap, swap, high, high, low], 0)


def halves(x):
    high = x.astype(jnp.bfloat16)
    return high, (x - high.astype(jnp.float32)).astype(jnp.bfloat16)


def pair_of(lane):
    return ((lane + 1) // 2) % (LANES // 2)


def planes(maps, det):
    j = det[...]
    m00, m01, m10, m11 = maps[0], maps[1], maps[2], maps[3]
    return j, j * node_weights(), (m00, m01, m10, m11), (j * m00, j * m01, j * m10, j * m11)


def dynamics_kernel(
    n_share, n_fields, air_in, heat_in, thick_in, ground_in, maps_in, det_in, table_in, tracer_in,
    w_out, packed_out, share_out, first_out, second_out, mass_out, table_out, tracer_out,
    air, heat, thick, ground, maps, det, sems,
):
    levels = heat.shape[0]
    copies = [
        pltpu.make_async_copy(source, held, sems.at[i])
        for i, (source, held) in enumerate(
            (
                (maps_in, maps), (det_in, det), (ground_in, ground), (heat_in, heat), (thick_in, thick), (air_in, air),
                (table_in, table_out), (tracer_in, tracer_out),
            )
        )
    ]
    for copy in copies:
        copy.start()
    for copy in copies[:-2]:
        copy.wait()
    row, lane = iota(0), iota(1)
    pair = pair_of(lane)
    j, mass, (m00, m01, m10, m11), (j00, j01, j10, j11) = planes(maps, det)
    scale = time_step * node_weights()
    undo = 1.0 / scale
    b11 = (j00 * m00 + j01 * m01) * undo
    b12 = (j00 * m10 + j01 * m11) * undo
    b22 = (j10 * m10 + j11 * m11) * undo
    along_rows = derivative_terms(0, scale)
    along_columns = derivative_terms(1, scale)
    ground_plane = ground[...]
    row_scale = time_step * by_node(row, WEIGHTS)

    def flux(first, second):
        return derive(first, 0, along_rows) + derive(second, 1, along_columns)

    def one_level(level, slot, below, speed, damp, packed):
        u, v = air[0, level], air[1, level]
        heat_l, thick_l = heat[level], thick[level]
        term = heat_l * thick_l
        square = u * u + v * v
        energy = 0.5 * square + (ground_plane + below + 0.5 * term)
        below = below + term
        speed = jnp.maximum(speed, square)
        first, second = j00 * u + j01 * v, j10 * u + j11 * v
        first_out[level] = first
        second_out[level] = second * row_scale
        rows, columns = derive(energy, 0, along_rows), derive(energy, 1, along_columns)
        new = [mass * u - (j00 * rows + j10 * columns), mass * v - (j01 * rows + j11 * columns)]
        rows, columns = derive(heat_l, 0, along_rows), derive(heat_l, 1, along_columns)
        new.append(mass * heat_l - (first * rows + second * columns))
        rows, columns = derive(thick_l, 0, along_rows), derive(thick_l, 1, along_columns)
        laplace = flux(b11 * rows + b12 * columns, b12 * rows + b22 * columns)
        damp = jnp.maximum(damp, jnp.abs(laplace))
        new.append(mass * thick_l - flux(thick_l * first, thick_l * second) + viscosity * laplace)
        for field, x in enumerate(new):
            x = sum_in_block(x)
            w_out[tile_of(field * levels + level), :] = x
            packed = jnp.where(pair == slot + field, pltpu.roll(x, 2 * (slot + field), 1), packed)
        return below, speed, damp, packed

    packed_mass = pltpu.roll(sum_in_block(mass), 4 * n_fields, 1)

    def one(turn, carry):
        half = levels // 2 - 1 - turn
        packed = jnp.where(pair == 2 * n_fields, packed_mass, 0.0)
        *carry, packed = one_level(2 * half + 1, n_fields, *carry, packed)
        *carry, packed = one_level(2 * half, 0, *carry, packed)
        packed_out[tile_of(half), :] = packed
        return tuple(carry)

    zero = jnp.zeros((ROWS, LANES), jnp.float32)
    total, speed, damp = lax.fori_loop(0, levels // 2, one, (zero, zero, zero), unroll=3)
    spacing = jnp.sqrt(m00 * m00 + m01 * m01 + m10 * m10 + m11 * m11)
    courant = jnp.max(time_step * jnp.sqrt(speed) * spacing, axis=0, keepdims=True)
    damping = jnp.max(damp * (viscosity / mass), axis=0, keepdims=True)
    bounds = jnp.where(row == 0, courant, damping)
    for peer in range(n_share):
        share_out[peer, pl.ds(0, ROWS), :] = total
        share_out[peer, pl.ds(ROWS, ROWS), :] = bounds
    mass_out[...] = mass
    for copy in copies[-2:]:
        copy.wait()


def tracer_kernel(firsts, seconds, mass_in, table, tracer, before, w_out, packed_out):
    tracers, levels = tracer.shape[:2]
    n_fields = 4 + tracers
    pair = pair_of(iota(1))
    mass = mass_in[...]
    along_rows = derivative_terms(0, time_step * node_weights())

    def one(half, _):
        packed = before[tile_of(half), :]
        plain, fluxes = [], []
        for level in (2 * half, 2 * half + 1):
            first, second = firsts[level], seconds[level]
            for t in range(tracers):
                q = tracer[t, level]
                plain.append(mass * q - derive(q * first, 0, along_rows))
                fluxes.append(q * second)
        high, low = halves(jnp.concatenate(plain, axis=0))
        swapped = jnp.dot(
            jnp.concatenate([high, low], axis=1), table[pl.ds(0, 2 * LANES), :], preferred_element_type=jnp.float32
        )
        high, low = halves(jnp.concatenate(fluxes, axis=0))
        derived = jnp.dot(
            jnp.concatenate([high, low, high], axis=1), table[pl.ds(2 * LANES, 3 * LANES), :],
            preferred_element_type=jnp.float32,
        )
        for i, x in enumerate(plain):
            part, t = i // tracers, i % tracers
            at = slice(i * ROWS, i * ROWS + ROWS)
            x = x + swapped[at] + derived[at]
            x = x + beside_in_block(x, 0)
            w_out[tile_of(t * levels + 2 * half + part), :] = x
            slot = part * n_fields + 4 + t
            packed = jnp.where(pair == slot, pltpu.roll(x, 2 * slot, 1), packed)
        packed_out[tile_of(half), :] = packed
        return 0

    lax.fori_loop(0, levels // 2, one, 0, unroll=3)
    tiles = tracers * levels
    w_out[pl.ds(tiles * ROWS, ROWS), :] = sum_in_block(mass)
    spare = w_out.shape[0] - (tiles + 1) * ROWS
    w_out[pl.ds((tiles + 1) * ROWS, spare), :] = jnp.zeros((spare, LANES), jnp.float32)


def carry_kernel(levels, n_lev, shared, dynamics, w, packed, maps, det, wind_out, far_out, near_out, packed_out, bound_out):
    lev, core = lax.axis_index("lev"), lax.axis_index("tile_1")
    odd = lax.rem(lax.axis_index(FACE), 2) == 1
    higher = jnp.zeros((ROWS, LANES), jnp.float32)
    bounds = shared[0, pl.ds(ROWS, ROWS), :]
    for peer in range(shared.shape[0]):
        counts = (peer // n_lev == core) & (peer % n_lev > lev)
        higher = higher + jnp.where(counts, shared[peer, pl.ds(0, ROWS), :], 0.0)
        bounds = jnp.maximum(bounds, shared[peer, pl.ds(ROWS, ROWS), :])
    lane = iota(1)
    pair = pair_of(lane)
    both = jnp.maximum(bounds, pltpu.roll(bounds, LANES // 2, 1))
    line = jnp.where(lane[0:1] < LANES // 2, both[0:1], both[1:2])
    bound_out[...] = jnp.broadcast_to(line[None], bound_out.shape)

    scale = time_step * node_weights()
    j = det[...]
    rows = derive(higher, 0, derivative_terms(0, scale))
    columns = derive(higher, 1, derivative_terms(1, scale))
    add_u = sum_in_block(-j * (maps[0] * rows + maps[2] * columns))
    add_v = sum_in_block(-j * (maps[1] * rows + maps[3] * columns))
    for field, add in ((0, add_u), (1, add_v)):
        for level in range(levels):
            at = pl.ds((field * levels + level) * ROWS, ROWS)
            wind_out[at, :] = dynamics[at, :] + add
    halves_of_levels = packed.shape[0] // ROWS
    corner_rows = 2 * ROWS
    edge_rows = far_out.shape[0] - corner_rows
    held = 4 * levels
    for start in range(0, edge_rows, ROWS):
        source, place = (dynamics, start * ROWS) if start < held else (w, (start - held) * ROWS)
        last = source[pl.ds(place + ROWS - 1, ROWS, stride=ROWS), :]
        first = source[pl.ds(place, ROWS, stride=ROWS), :]
        far_out[pl.ds(start, ROWS), :] = jnp.where(odd, last, first)
        near_out[pl.ds(start, ROWS), :] = jnp.where(odd, first, last)
    for out, ends in ((far_out, odd), (near_out, jnp.logical_not(odd))):
        for start, add in ((0, add_u), (levels, add_v)):
            at = pl.ds(start, levels)
            out[at, :] = out[at, :] + jnp.where(ends, add[ROWS - 1 : ROWS], add[0:1])
        out[pl.ds(edge_rows, corner_rows), :] = jnp.zeros((corner_rows, LANES), jnp.float32)
    n_fields = 4 + (w.shape[0] // ROWS - 1) // levels
    add = jnp.zeros((ROWS, LANES), jnp.float32)
    for slot in (0, n_fields):
        add = jnp.where(pair == slot, pltpu.roll(add_u, 2 * slot, 1), add)
        add = jnp.where(pair == slot + 1, pltpu.roll(add_v, 2 * slot + 2, 1), add)
    for half in range(halves_of_levels):
        at = pl.ds(half * ROWS, ROWS)
        x = packed[at, :] + add
        packed_out[at, :] = x
        for out, ends in ((far_out, odd), (near_out, jnp.logical_not(odd))):
            out[pl.ds(edge_rows + half, 1), :] = jnp.where(ends, x[ROWS - 1 : ROWS], x[0:1])


def cosine_sine(code):
    cosine = jnp.where(code == 0, 1.0, jnp.where(code == 2, -1.0, 0.0)).astype(jnp.float32)
    sine = jnp.where(code == 1, 1.0, jnp.where(code == 3, -1.0, 0.0)).astype(jnp.float32)
    return cosine, sine


def turned(u, v, code):
    cosine, sine = cosine_sine(code)
    return cosine * u - sine * v, sine * u + cosine * v


def sum_kernel(
    levels, n_face, n_tile, rotations, flips, valences, w, dynamics, wind, far, near, inside, outside,
    air_out, heat_out, thick_out, tracer_out, up_rim, down_rim, side_rim,
    air_held, heat_held, thick_held, tracer_held, out_sem,
):
    face, tile = lax.axis_index(FACE), lax.axis_index(TILE)
    face_lower = lax.rem(face + n_face - 1, n_face)
    tile_lower = lax.rem(tile + n_tile - 1, n_tile)

    def at(f, t):
        return f * n_tile + t

    top_code = (4 - rotations[2 * at(face_lower, tile)]) & 3
    bottom_code = rotations[2 * at(face, tile)]
    west_code = (4 - rotations[2 * at(face, tile_lower) + 1]) & 3
    east_code = rotations[2 * at(face, tile) + 1]
    top_flip = flips[2 * at(face_lower, tile)]
    bottom_flip = flips[2 * at(face, tile)]
    west_flip = flips[2 * at(face, tile_lower) + 1]
    east_flip = flips[2 * at(face, tile) + 1]
    corners = {
        ("up", "west"): valences[at(face_lower, tile_lower)],
        ("up", "east"): valences[at(face_lower, tile)],
        ("down", "west"): valences[at(face, tile_lower)],
        ("down", "east"): valences[at(face, tile)],
    }
    row, lane = iota(0), iota(1)
    pair = pair_of(lane)
    tracers = tracer_out.shape[0]
    fields = 4 + tracers
    count = side_rim.shape[0]

    edge_rows = up_rim.shape[0]
    odd_face, odd_tile = lax.rem(face, 2) == 1, lax.rem(tile, 2) == 1
    for out, flag, by_near in ((up_rim, top_flip, odd_face), (down_rim, bottom_flip, jnp.logical_not(odd_face))):
        places = jnp.where(flag == 1, LANES - 1 - lane, lane)
        for start in range(0, edge_rows, ROWS):
            rows = pl.ds(start, ROWS)
            x = jnp.where(by_near, near[rows, :], far[rows, :])
            out[rows, :] = jnp.take_along_axis(x, places, axis=1, mode="promise_in_bounds")

    within = jnp.where(pair >= fields, pair - fields, pair)
    is_u, is_v = (within == 0) & (pair < 2 * fields), within == 1

    def turn_packed(x, code):
        cosine, sine = cosine_sine(code)
        rows = x.shape[0]
        u, v = (jnp.broadcast_to(mask[0:1], (rows, LANES)) for mask in (is_u.astype(jnp.int32), is_v.astype(jnp.int32)))
        from_v, from_u = pltpu.roll(x, LANES - 2, 1), pltpu.roll(x, 2, 1)
        return jnp.where(u == 1, cosine * x - sine * from_v, jnp.where(v == 1, sine * from_u + cosine * x, x))

    def side(from_inside, flag, code, name):
        def rows_at(start, rows):
            at = pl.ds(start, rows)
            return jnp.where(from_inside, inside[at, :], outside[at, :])

        far_end, near_end = rows_at(count * ROWS, 2 * ROWS), rows_at((count + 2) * ROWS, 2 * ROWS)
        ends = []
        for end, row_code, by_near in (("up", top_code, odd_face), ("down", bottom_code, jnp.logical_not(odd_face))):
            corner = turn_packed(jnp.where(by_near, near_end, far_end), (row_code + code) & 3)
            ends.append(jnp.where(corners[end, name] == 4, corner, 0.0))
        columns = []
        for half in range(count):
            start = half * ROWS
            x = jnp.concatenate(
                [rows_at(start + jnp.where(flag == 1, ROWS - 1 - r, r), 1) for r in range(ROWS)], axis=0
            )
            x = turn_packed(x, code)
            over = [jnp.broadcast_to(end[half : half + 1], (ROWS, LANES)) for end in ends]
            columns.append(x + jnp.where(row == 0, over[0], jnp.where(row == ROWS - 1, over[1], 0.0)))
        return columns

    wests = side(odd_tile, west_flip, west_code, "west")
    easts = side(jnp.logical_not(odd_tile), east_flip, east_code, "east")
    for half in range(count):
        side_rim[half] = jnp.where(lane % 2 == 0, pltpu.roll(wests[half], 1, 1), pltpu.roll(easts[half], LANES - 1, 1))

    at_side = (lane == 0) | (lane == LANES - 1)

    def summed(x, upper, lower, sides, slot):
        x = x + jnp.where(row == 0, upper, jnp.where(row == ROWS - 1, lower, 0.0))
        moved = pltpu.roll(sides, (LANES - 2 * slot) % LANES, 1) if slot else sides
        return x + jnp.where(at_side, moved, 0.0)

    def rim(ref, index):
        return jnp.broadcast_to(ref[pl.ds(index, 1), :], (ROWS, LANES))

    index = fields * levels
    mass = summed(w[pl.ds((index - 4 * levels) * ROWS, ROWS), :], rim(up_rim, index), rim(down_rim, index), side_rim[0], 2 * fields)
    scale = 1.0 / mass

    def one(half, _):
        sides = side_rim[half]
        for part in range(2):
            level, slot = 2 * half + part, part * fields
            u_at, v_at = level, levels + level
            upper = turned(rim(up_rim, u_at), rim(up_rim, v_at), top_code)
            lower = turned(rim(down_rim, u_at), rim(down_rim, v_at), bottom_code)
            air_held[0, level] = summed(wind[tile_of(u_at), :], upper[0], lower[0], sides, slot) * scale
            air_held[1, level] = summed(wind[tile_of(v_at), :], upper[1], lower[1], sides, slot + 1) * scale
            for field in range(2, fields):
                index = field * levels + level
                x = dynamics[tile_of(index), :] if field < 4 else w[tile_of(index - 4 * levels), :]
                x = summed(x, rim(up_rim, index), rim(down_rim, index), sides, slot + field) * scale
                if field == 2:
                    heat_held[level] = x
                elif field == 3:
                    thick_held[level] = x
                else:
                    tracer_held[field - 4, level] = x
            for copy in copies_out(level):
                copy.start()
        return 0

    def copies_out(level):
        return (
            pltpu.make_async_copy(air_held.at[:, level], air_out.at[:, level], out_sem.at[0, level]),
            pltpu.make_async_copy(heat_held.at[level], heat_out.at[level], out_sem.at[1, level]),
            pltpu.make_async_copy(thick_held.at[level], thick_out.at[level], out_sem.at[2, level]),
            pltpu.make_async_copy(tracer_held.at[:, level], tracer_out.at[:, level], out_sem.at[3, level]),
        )

    def finish(level, _):
        for copy in copies_out(level):
            copy.wait()
        return 0

    lax.fori_loop(0, levels // 2, one, 0)
    lax.fori_loop(0, levels, finish, 0)


def swap_pairs(x, axes, start):
    count = lax.axis_size(axes)
    pairs = [(i % count, (i + 1) % count) for i in range(start, count + start, 2)]
    return lax.ppermute(x, axes, pairs + [(j, i) for i, j in pairs])


def bounds_kernel(plane, out):
    both = jnp.max(plane[...], axis=0)
    lane = lax.broadcasted_iota(jnp.int32, (1, LANES), 1)
    for i in range(2):
        out[i] = jnp.max(jnp.where(lane // (LANES // 2) == i, both, 0.0))


def on_device(air, heat, thick, tracer, ground, maps, det, rotations, flips, valences):
    levels = heat.shape[0]
    tracers = tracer.shape[0]
    fields = 4 + tracers
    edge_rows = -(-(fields * levels + 1) // ROWS) * ROWS
    count = levels // 2
    n_lev = lax.axis_size("lev")
    n_share = lax.axis_size(COLUMN)
    n_face, n_tile = lax.axis_size(FACE), lax.axis_size(TILE)
    n_plane = lax.axis_size(PLANE)

    def f32(*shape):
        return jax.ShapeDtypeStruct(shape, jnp.float32)

    def in_hbm(x):
        return pltpu.with_memory_space_constraint(x, pltpu.HBM)

    inputs = tuple(in_hbm(x) for x in (air, heat, thick, ground, maps, det, jnp.asarray(lane_tables()), tracer))
    params = pltpu.CompilerParams(vmem_limit_bytes=24 * 1024 * 1024)
    dynamics, packed, share, *for_tracers = pl.pallas_call(
        lambda *refs: dynamics_kernel(n_share, fields, *refs),
        out_shape=(
            f32(4 * levels * ROWS, LANES),
            f32(count * ROWS, LANES),
            f32(n_share, 2 * ROWS, LANES),
            f32(levels, ROWS, LANES),
            f32(levels, ROWS, LANES),
            f32(ROWS, LANES),
            jax.ShapeDtypeStruct(inputs[6].shape, inputs[6].dtype),
            f32(*tracer.shape),
        ),
        in_specs=[ANY] * 8,
        out_specs=(VMEM,) * 8,
        scratch_shapes=[pltpu.VMEM(x.shape, x.dtype) for x in inputs[:6]] + [pltpu.SemaphoreType.DMA((8,))],
        compiler_params=params,
        name="dynamics",
    )(*inputs)
    shared = lax.all_to_all(share, COLUMN, 0, 0, tiled=True)
    w, packed = pl.pallas_call(
        tracer_kernel,
        out_shape=(f32((edge_rows - 4 * levels) * ROWS, LANES), f32(count * ROWS, LANES)),
        in_specs=[VMEM] * 6,
        out_specs=(VMEM,) * 2,
        compiler_params=params,
        name="tracers",
    )(*for_tracers, packed)
    wind, far, near, packed, bound = pl.pallas_call(
        lambda *refs: carry_kernel(levels, n_lev, *refs),
        out_shape=(
            f32(2 * levels * ROWS, LANES),
            f32(edge_rows + 2 * ROWS, LANES),
            f32(edge_rows + 2 * ROWS, LANES),
            f32(count * ROWS, LANES),
            f32(n_plane, 1, LANES),
        ),
        in_specs=[VMEM] * 6,
        out_specs=(VMEM,) * 5,
        compiler_params=params,
        name="carry",
    )(shared, dynamics, w, packed, maps, det)
    far = swap_pairs(far, FACE, 1)
    near = swap_pairs(near, FACE, 0)
    plane = lax.all_to_all(bound, PLANE, 0, 0, tiled=True)
    stepping_bounds = pl.pallas_call(
        bounds_kernel, out_shape=f32(2), in_specs=[VMEM], out_specs=SMEM, compiler_params=params, name="bounds"
    )(plane)
    sides = jnp.concatenate([packed, far[edge_rows:], near[edge_rows:]], 0)
    inside = swap_pairs(sides, TILE, 0)
    outside = swap_pairs(sides, TILE, 1)
    sums = pl.pallas_call(
        lambda *refs: sum_kernel(levels, n_face, n_tile, *refs),
        out_shape=(f32(*air.shape), f32(*heat.shape), f32(*thick.shape), f32(*tracer.shape)),
        in_specs=[SMEM] * 3 + [VMEM] * 7,
        out_specs=(ANY,) * 4,
        scratch_shapes=[
            pltpu.VMEM((edge_rows, LANES), jnp.float32),
            pltpu.VMEM((edge_rows, LANES), jnp.float32),
            pltpu.VMEM((count, ROWS, LANES), jnp.float32),
            *(pltpu.VMEM(x.shape, jnp.float32) for x in (air, heat, thick, tracer)),
            pltpu.SemaphoreType.DMA((4, levels)),
        ],
        compiler_params=params,
        name="sum",
    )
    air_next, heat_next, thick_next, tracer_next = sums(rotations.reshape(-1), flips.reshape(-1), valences.reshape(-1), w, dynamics, wind, far, near, inside, outside)
    return air_next, heat_next, thick_next, tracer_next, stepping_bounds


def solution(mesh):
    face, tile, lev = mesh.shape["face"], mesh.shape["tile"], mesh.shape["lev"]
    inner = min(face, 4)
    split = Mesh(
        mesh.devices.reshape(face // inner, inner, tile // 2, 2, lev),
        ("face_0", "face_1", "tile_0", "tile_1", "lev"),
    )
    level_plane = P("lev", FACE, TILE)
    field_level_plane = P(None, "lev", FACE, TILE)
    return jax.shard_map(
        on_device,
        mesh=split,
        in_specs=(
            field_level_plane, level_plane, level_plane, field_level_plane,
            P(FACE, TILE), P(None, FACE, TILE), P(FACE, TILE), P(), P(), P(),
        ),
        out_specs=(field_level_plane, level_plane, level_plane, field_level_plane, P()),
        check_vma=False,
    )
```

```python
import math

import jax
import jax.numpy as jnp
import numpy as np
from jax import lax
from jax.experimental import pallas as pl
from jax.experimental.pallas import tpu as pltpu
from jax.sharding import Mesh
from jax.sharding import PartitionSpec as P


FACE = ("face_0", "face_1")
TILE = ("tile_0", "tile_1")
PLANE = FACE + ("tile_0",)
COLUMN = ("tile_1", "lev")

time_step = 0.05
viscosity = 0.05

ROWS, LANES = 8, 128
VMEM = pl.BlockSpec(memory_space=pltpu.VMEM)
ANY = pl.BlockSpec(memory_space=pltpu.HBM)
SMEM = pl.BlockSpec(memory_space=pltpu.SMEM)


def gll_tables():
    offset = 1.0 / math.sqrt(5.0)
    nodes = np.array([-1.0, -offset, offset, 1.0])
    weights = np.array([1.0 / 6.0, 5.0 / 6.0, 5.0 / 6.0, 1.0 / 6.0])
    bary = np.ones(4)
    for i in range(4):
        for j in range(4):
            if j != i:
                bary[i] = bary[i] / (nodes[i] - nodes[j])
    derivative = np.zeros((4, 4))
    for i in range(4):
        for j in range(4):
            if j != i:
                derivative[i, j] = bary[j] / bary[i] / (nodes[i] - nodes[j])
        derivative[i, i] = -np.sum(derivative[i])
    return derivative, weights


DERIVATIVE, WEIGHTS = gll_tables()


def iota(axis):
    return lax.broadcasted_iota(jnp.int32, (ROWS, LANES), axis)


def by_node(place, values):
    node = place % 4
    plane = jnp.full((ROWS, LANES), float(values[0]), jnp.float32)
    for i in range(1, 4):
        plane = jnp.where(node == i, float(values[i]), plane)
    return plane


def node_weights():
    return by_node(iota(0), WEIGHTS) * by_node(iota(1), WEIGHTS)


def derivative_terms(axis, scale):
    place = iota(axis)
    terms = []
    for k in range(-3, 4):
        values = [DERIVATIVE[i, i + k] if 0 <= i + k < 4 else 0.0 for i in range(4)]
        terms.append((k, by_node(place, values) * scale))
    return terms


def derive(field, axis, terms):
    size = field.shape[axis]
    total = None
    for k, coefficient in terms:
        moved = field if k == 0 else pltpu.roll(field, (-k) % size, axis)
        part = coefficient * moved
        total = part if total is None else total + part
    return total


def tile_of(index):
    return pl.ds(pl.multiple_of(index * ROWS, ROWS), ROWS)


def beside_in_block(x, axis):
    place, size = iota(axis), x.shape[axis]
    later, earlier = pltpu.roll(x, size - 1, axis), pltpu.roll(x, 1, axis)
    before_border = (place % 4 == 3) & (place < size - 1)
    after_border = (place % 4 == 0) & (place > 0)
    return jnp.where(before_border, later, jnp.where(after_border, earlier, 0.0))


def sum_in_block(x):
    x = x + beside_in_block(x, 1)
    return x + beside_in_block(x, 0)


def lane_tables():
    swap = np.zeros((LANES, LANES))
    for c in range(3, LANES - 1, 4):
        swap[c, c + 1] = swap[c + 1, c] = 1.0
    derive_columns = np.kron(np.eye(LANES // 4), (WEIGHTS[:, None] * DERIVATIVE).T)
    full = -(derive_columns @ (np.eye(LANES) + swap)).astype(np.float32)
    high = full.astype(jnp.bfloat16)
    low = (full - high.astype(np.float32)).astype(jnp.bfloat16)
    swap = swap.astype(jnp.bfloat16)
    return np.concatenate([swap, swap, high, high, low], 0)


def halves(x):
    high = x.astype(jnp.bfloat16)
    return high, (x - high.astype(jnp.float32)).astype(jnp.bfloat16)


def pair_of(lane):
    return ((lane + 1) // 2) % (LANES // 2)


def planes(maps, det):
    j = det[...]
    m00, m01, m10, m11 = maps[0], maps[1], maps[2], maps[3]
    return j, j * node_weights(), (m00, m01, m10, m11), (j * m00, j * m01, j * m10, j * m11)


def column_kernel(n_share, *refs):
    air_in, heat_in, thick_in, ground_in, maps_in, det_in, table_in = refs[:7]
    share_out, levels_out, planes_out, table, sems = refs[7:]
    levels = levels_out.shape[1]
    air, heat, thick = levels_out.at[pl.ds(3, 2)], levels_out.at[5], levels_out.at[6]
    maps, det, ground = planes_out.at[pl.ds(0, 4)], planes_out.at[4], planes_out.at[5]
    copies = [
        pltpu.make_async_copy(source, held, sems.at[i])
        for i, (source, held) in enumerate(
            (
                (maps_in, maps), (det_in, det), (thick_in, thick), (heat_in, heat), (air_in, air),
                (ground_in, ground), (table_in, table),
            )
        )
    ]
    for copy in copies:
        copy.start()
    for copy in copies[:-2]:
        copy.wait()
    row = iota(0)
    _, mass, (m00, m01, m10, m11), (j00, j01, j10, j11) = planes(maps, det)
    scale = time_step * node_weights()
    undo = 1.0 / scale
    b11 = (j00 * m00 + j01 * m01) * undo
    b12 = (j00 * m10 + j01 * m11) * undo
    b22 = (j10 * m10 + j11 * m11) * undo
    along_rows = derivative_terms(0, scale)
    along_columns = derivative_terms(1, scale)
    row_scale = time_step * by_node(row, WEIGHTS)

    def one(level, carry):
        total, speed, damp = carry
        u, v, thick_l = air[0, level], air[1, level], thick[level]
        total = total + heat[level] * thick_l
        speed = jnp.maximum(speed, u * u + v * v)
        levels_out[0, level] = j00 * u + j01 * v
        levels_out[1, level] = (j10 * u + j11 * v) * row_scale
        rows, columns = derive(thick_l, 0, along_rows), derive(thick_l, 1, along_columns)
        laplace = derive(b11 * rows + b12 * columns, 0, along_rows) + derive(b12 * rows + b22 * columns, 1, along_columns)
        levels_out[2, level] = laplace
        return total, speed, jnp.maximum(damp, jnp.abs(laplace))

    zero = jnp.zeros((ROWS, LANES), jnp.float32)
    total, speed, damp = lax.fori_loop(0, levels, one, (zero, zero, zero), unroll=6)
    spacing = jnp.sqrt(m00 * m00 + m01 * m01 + m10 * m10 + m11 * m11)
    courant = jnp.max(time_step * jnp.sqrt(speed) * spacing, axis=0, keepdims=True)
    damping = jnp.max(damp * (viscosity / mass), axis=0, keepdims=True)
    bounds = jnp.where(row == 0, courant, damping)
    for peer in range(n_share):
        share_out[peer, pl.ds(0, ROWS), :] = total
        share_out[peer, pl.ds(ROWS, ROWS), :] = bounds
    planes_out[6] = mass
    for copy in copies[-2:]:
        copy.wait()


def fields_kernel(by_level, by_point, table, tracer_in, dynamics_out, w_out, packed_out, tracer, sem):
    copy = pltpu.make_async_copy(tracer_in, tracer, sem.at[0])
    copy.start()
    firsts, seconds, laplaces = by_level.at[0], by_level.at[1], by_level.at[2]
    air, heat, thick = by_level.at[pl.ds(3, 2)], by_level.at[5], by_level.at[6]
    maps, det, ground = by_point.at[pl.ds(0, 4)], by_point.at[4], by_point.at[5]
    dynamics(firsts, laplaces, air, heat, thick, ground, maps, det, tracer, dynamics_out, packed_out)
    copy.wait()
    tracers_of(firsts, seconds, by_point[6], table, tracer, packed_out, w_out, packed_out)


def dynamics(firsts, laplaces, air, heat, thick, ground, maps, det, tracer, w_out, packed_out):
    levels = heat.shape[0]
    n_fields = 4 + tracer.shape[0]
    lane = iota(1)
    pair = pair_of(lane)
    _, mass, _, (j00, j01, j10, j11) = planes(maps, det)
    scale = time_step * node_weights()
    along_rows = derivative_terms(0, scale)
    along_columns = derivative_terms(1, scale)
    ground_plane = ground[...]

    def flux(first, second):
        return derive(first, 0, along_rows) + derive(second, 1, along_columns)

    def one_level(level, slot, below, packed):
        u, v = air[0, level], air[1, level]
        heat_l, thick_l = heat[level], thick[level]
        term = heat_l * thick_l
        energy = 0.5 * (u * u + v * v) + (ground_plane + below + 0.5 * term)
        first, second = firsts[level], j10 * u + j11 * v
        rows, columns = derive(energy, 0, along_rows), derive(energy, 1, along_columns)
        new = [mass * u - (j00 * rows + j10 * columns), mass * v - (j01 * rows + j11 * columns)]
        rows, columns = derive(heat_l, 0, along_rows), derive(heat_l, 1, along_columns)
        new.append(mass * heat_l - (first * rows + second * columns))
        new.append(mass * thick_l - flux(thick_l * first, thick_l * second) + viscosity * laplaces[level])
        for field, x in enumerate(new):
            x = sum_in_block(x)
            w_out[tile_of(field * levels + level), :] = x
            packed = jnp.where(pair == slot + field, pltpu.roll(x, 2 * (slot + field), 1), packed)
        return below + term, packed

    packed_mass = pltpu.roll(sum_in_block(mass), 4 * n_fields, 1)

    def one(turn, below):
        half = levels // 2 - 1 - turn
        packed = jnp.where(pair == 2 * n_fields, packed_mass, 0.0)
        below, packed = one_level(2 * half + 1, n_fields, below, packed)
        below, packed = one_level(2 * half, 0, below, packed)
        packed_out[tile_of(half), :] = packed
        return below

    lax.fori_loop(0, levels // 2, one, jnp.zeros((ROWS, LANES), jnp.float32), unroll=3)


def tracers_of(firsts, seconds, mass, table, tracer, before, w_out, packed_out):
    tracers, levels = tracer.shape[:2]
    n_fields = 4 + tracers
    pair = pair_of(iota(1))
    along_rows = derivative_terms(0, time_step * node_weights())

    def one(half, _):
        packed = before[tile_of(half), :]
        plain, fluxes = [], []
        for level in (2 * half, 2 * half + 1):
            first, second = firsts[level], seconds[level]
            for t in range(tracers):
                q = tracer[t, level]
                plain.append(mass * q - derive(q * first, 0, along_rows))
                fluxes.append(q * second)
        high, low = halves(jnp.concatenate(plain, axis=0))
        swapped = jnp.dot(
            jnp.concatenate([high, low], axis=1), table[pl.ds(0, 2 * LANES), :], preferred_element_type=jnp.float32
        )
        high, low = halves(jnp.concatenate(fluxes, axis=0))
        derived = jnp.dot(
            jnp.concatenate([high, low, high], axis=1), table[pl.ds(2 * LANES, 3 * LANES), :],
            preferred_element_type=jnp.float32,
        )
        for i, x in enumerate(plain):
            part, t = i // tracers, i % tracers
            at = slice(i * ROWS, i * ROWS + ROWS)
            x = x + swapped[at] + derived[at]
            x = x + beside_in_block(x, 0)
            w_out[tile_of(t * levels + 2 * half + part), :] = x
            slot = part * n_fields + 4 + t
            packed = jnp.where(pair == slot, pltpu.roll(x, 2 * slot, 1), packed)
        packed_out[tile_of(half), :] = packed
        return 0

    lax.fori_loop(0, levels // 2, one, 0, unroll=3)
    tiles = tracers * levels
    w_out[pl.ds(tiles * ROWS, ROWS), :] = sum_in_block(mass)
    spare = w_out.shape[0] - (tiles + 1) * ROWS
    w_out[pl.ds((tiles + 1) * ROWS, spare), :] = jnp.zeros((spare, LANES), jnp.float32)


def carry_kernel(levels, n_lev, shared, dynamics, w, packed, maps, det, wind_out, far_out, near_out, packed_out, bound_out):
    lev, core = lax.axis_index("lev"), lax.axis_index("tile_1")
    odd = lax.rem(lax.axis_index(FACE), 2) == 1
    higher = jnp.zeros((ROWS, LANES), jnp.float32)
    bounds = shared[0, pl.ds(ROWS, ROWS), :]
    for peer in range(shared.shape[0]):
        counts = (peer // n_lev == core) & (peer % n_lev > lev)
        higher = higher + jnp.where(counts, shared[peer, pl.ds(0, ROWS), :], 0.0)
        bounds = jnp.maximum(bounds, shared[peer, pl.ds(ROWS, ROWS), :])
    lane = iota(1)
    pair = pair_of(lane)
    both = jnp.maximum(bounds, pltpu.roll(bounds, LANES // 2, 1))
    line = jnp.where(lane[0:1] < LANES // 2, both[0:1], both[1:2])
    bound_out[...] = jnp.broadcast_to(line[None], bound_out.shape)

    scale = time_step * node_weights()
    j = det[...]
    rows = derive(higher, 0, derivative_terms(0, scale))
    columns = derive(higher, 1, derivative_terms(1, scale))
    add_u = sum_in_block(-j * (maps[0] * rows + maps[2] * columns))
    add_v = sum_in_block(-j * (maps[1] * rows + maps[3] * columns))
    for field, add in ((0, add_u), (1, add_v)):
        for level in range(levels):
            at = pl.ds((field * levels + level) * ROWS, ROWS)
            wind_out[at, :] = dynamics[at, :] + add
    halves_of_levels = packed.shape[0] // ROWS
    corner_rows = 2 * ROWS
    edge_rows = far_out.shape[0] - corner_rows
    held = 4 * levels
    for start in range(0, edge_rows, ROWS):
        source, place = (dynamics, start * ROWS) if start < held else (w, (start - held) * ROWS)
        last = source[pl.ds(place + ROWS - 1, ROWS, stride=ROWS), :]
        first = source[pl.ds(place, ROWS, stride=ROWS), :]
        far_out[pl.ds(start, ROWS), :] = jnp.where(odd, last, first)
        near_out[pl.ds(start, ROWS), :] = jnp.where(odd, first, last)
    for out, ends in ((far_out, odd), (near_out, jnp.logical_not(odd))):
        for start, add in ((0, add_u), (levels, add_v)):
            at = pl.ds(start, levels)
            out[at, :] = out[at, :] + jnp.where(ends, add[ROWS - 1 : ROWS], add[0:1])
        out[pl.ds(edge_rows, corner_rows), :] = jnp.zeros((corner_rows, LANES), jnp.float32)
    n_fields = 4 + (w.shape[0] // ROWS - 1) // levels
    add = jnp.zeros((ROWS, LANES), jnp.float32)
    for slot in (0, n_fields):
        add = jnp.where(pair == slot, pltpu.roll(add_u, 2 * slot, 1), add)
        add = jnp.where(pair == slot + 1, pltpu.roll(add_v, 2 * slot + 2, 1), add)
    for half in range(halves_of_levels):
        at = pl.ds(half * ROWS, ROWS)
        x = packed[at, :] + add
        packed_out[at, :] = x
        for out, ends in ((far_out, odd), (near_out, jnp.logical_not(odd))):
            out[pl.ds(edge_rows + half, 1), :] = jnp.where(ends, x[ROWS - 1 : ROWS], x[0:1])


def cosine_sine(code):
    cosine = jnp.where(code == 0, 1.0, jnp.where(code == 2, -1.0, 0.0)).astype(jnp.float32)
    sine = jnp.where(code == 1, 1.0, jnp.where(code == 3, -1.0, 0.0)).astype(jnp.float32)
    return cosine, sine


def turned(u, v, code):
    cosine, sine = cosine_sine(code)
    return cosine * u - sine * v, sine * u + cosine * v


def sum_kernel(
    levels, n_face, n_tile, rotations, flips, valences, w, dynamics, wind, far, near, inside, outside,
    air_out, heat_out, thick_out, tracer_out, up_rim, down_rim, side_rim,
    air_held, heat_held, thick_held, tracer_held, out_sem,
):
    face, tile = lax.axis_index(FACE), lax.axis_index(TILE)
    face_lower = lax.rem(face + n_face - 1, n_face)
    tile_lower = lax.rem(tile + n_tile - 1, n_tile)

    def at(f, t):
        return f * n_tile + t

    top_code = (4 - rotations[2 * at(face_lower, tile)]) & 3
    bottom_code = rotations[2 * at(face, tile)]
    west_code = (4 - rotations[2 * at(face, tile_lower) + 1]) & 3
    east_code = rotations[2 * at(face, tile) + 1]
    top_flip = flips[2 * at(face_lower, tile)]
    bottom_flip = flips[2 * at(face, tile)]
    west_flip = flips[2 * at(face, tile_lower) + 1]
    east_flip = flips[2 * at(face, tile) + 1]
    corners = {
        ("up", "west"): valences[at(face_lower, tile_lower)],
        ("up", "east"): valences[at(face_lower, tile)],
        ("down", "west"): valences[at(face, tile_lower)],
        ("down", "east"): valences[at(face, tile)],
    }
    row, lane = iota(0), iota(1)
    pair = pair_of(lane)
    tracers = tracer_out.shape[0]
    fields = 4 + tracers
    count = side_rim.shape[0]

    edge_rows = up_rim.shape[0]
    odd_face, odd_tile = lax.rem(face, 2) == 1, lax.rem(tile, 2) == 1
    for out, flag, by_near in ((up_rim, top_flip, odd_face), (down_rim, bottom_flip, jnp.logical_not(odd_face))):
        places = jnp.where(flag == 1, LANES - 1 - lane, lane)
        for start in range(0, edge_rows, ROWS):
            rows = pl.ds(start, ROWS)
            x = jnp.where(by_near, near[rows, :], far[rows, :])
            out[rows, :] = jnp.take_along_axis(x, places, axis=1, mode="promise_in_bounds")

    within = jnp.where(pair >= fields, pair - fields, pair)
    is_u, is_v = (within == 0) & (pair < 2 * fields), within == 1

    def turn_packed(x, code):
        cosine, sine = cosine_sine(code)
        rows = x.shape[0]
        u, v = (jnp.broadcast_to(mask[0:1], (rows, LANES)) for mask in (is_u.astype(jnp.int32), is_v.astype(jnp.int32)))
        from_v, from_u = pltpu.roll(x, LANES - 2, 1), pltpu.roll(x, 2, 1)
        return jnp.where(u == 1, cosine * x - sine * from_v, jnp.where(v == 1, sine * from_u + cosine * x, x))

    def side(from_inside, flag, code, name):
        def rows_at(start, rows):
            at = pl.ds(start, rows)
            return jnp.where(from_inside, inside[at, :], outside[at, :])

        far_end, near_end = rows_at(count * ROWS, 2 * ROWS), rows_at((count + 2) * ROWS, 2 * ROWS)
        ends = []
        for end, row_code, by_near in (("up", top_code, odd_face), ("down", bottom_code, jnp.logical_not(odd_face))):
            corner = turn_packed(jnp.where(by_near, near_end, far_end), (row_code + code) & 3)
            ends.append(jnp.where(corners[end, name] == 4, corner, 0.0))
        columns = []
        for half in range(count):
            start = half * ROWS
            x = jnp.concatenate(
                [rows_at(start + jnp.where(flag == 1, ROWS - 1 - r, r), 1) for r in range(ROWS)], axis=0
            )
            x = turn_packed(x, code)
            over = [jnp.broadcast_to(end[half : half + 1], (ROWS, LANES)) for end in ends]
            columns.append(x + jnp.where(row == 0, over[0], jnp.where(row == ROWS - 1, over[1], 0.0)))
        return columns

    wests = side(odd_tile, west_flip, west_code, "west")
    easts = side(jnp.logical_not(odd_tile), east_flip, east_code, "east")
    for half in range(count):
        side_rim[half] = jnp.where(lane % 2 == 0, pltpu.roll(wests[half], 1, 1), pltpu.roll(easts[half], LANES - 1, 1))

    at_side = (lane == 0) | (lane == LANES - 1)

    def summed(x, upper, lower, sides, slot):
        x = x + jnp.where(row == 0, upper, jnp.where(row == ROWS - 1, lower, 0.0))
        moved = pltpu.roll(sides, (LANES - 2 * slot) % LANES, 1) if slot else sides
        return x + jnp.where(at_side, moved, 0.0)

    def rim(ref, index):
        return jnp.broadcast_to(ref[pl.ds(index, 1), :], (ROWS, LANES))

    index = fields * levels
    mass = summed(w[pl.ds((index - 4 * levels) * ROWS, ROWS), :], rim(up_rim, index), rim(down_rim, index), side_rim[0], 2 * fields)
    scale = 1.0 / mass

    def one(half, _):
        sides = side_rim[half]
        for part in range(2):
            level, slot = 2 * half + part, part * fields
            u_at, v_at = level, levels + level
            upper = turned(rim(up_rim, u_at), rim(up_rim, v_at), top_code)
            lower = turned(rim(down_rim, u_at), rim(down_rim, v_at), bottom_code)
            air_held[0, level] = summed(wind[tile_of(u_at), :], upper[0], lower[0], sides, slot) * scale
            air_held[1, level] = summed(wind[tile_of(v_at), :], upper[1], lower[1], sides, slot + 1) * scale
            for field in range(2, fields):
                index = field * levels + level
                x = dynamics[tile_of(index), :] if field < 4 else w[tile_of(index - 4 * levels), :]
                x = summed(x, rim(up_rim, index), rim(down_rim, index), sides, slot + field) * scale
                if field == 2:
                    heat_held[level] = x
                elif field == 3:
                    thick_held[level] = x
                else:
                    tracer_held[field - 4, level] = x
            for copy in copies_out(level):
                copy.start()
        return 0

    def copies_out(level):
        return (
            pltpu.make_async_copy(air_held.at[:, level], air_out.at[:, level], out_sem.at[0, level]),
            pltpu.make_async_copy(heat_held.at[level], heat_out.at[level], out_sem.at[1, level]),
            pltpu.make_async_copy(thick_held.at[level], thick_out.at[level], out_sem.at[2, level]),
            pltpu.make_async_copy(tracer_held.at[:, level], tracer_out.at[:, level], out_sem.at[3, level]),
        )

    def finish(level, _):
        for copy in copies_out(level):
            copy.wait()
        return 0

    lax.fori_loop(0, levels // 2, one, 0, unroll=3)
    lax.fori_loop(0, levels, finish, 0)


def swap_pairs(x, axes, start):
    count = lax.axis_size(axes)
    pairs = [(i % count, (i + 1) % count) for i in range(start, count + start, 2)]
    return lax.ppermute(x, axes, pairs + [(j, i) for i, j in pairs])


def bounds_kernel(plane, out):
    both = jnp.max(plane[...], axis=0)
    lane = lax.broadcasted_iota(jnp.int32, (1, LANES), 1)
    for i in range(2):
        out[i] = jnp.max(jnp.where(lane // (LANES // 2) == i, both, 0.0))


def on_device(air, heat, thick, tracer, ground, maps, det, rotations, flips, valences):
    levels = heat.shape[0]
    tracers = tracer.shape[0]
    fields = 4 + tracers
    edge_rows = -(-(fields * levels + 1) // ROWS) * ROWS
    count = levels // 2
    n_lev = lax.axis_size("lev")
    n_share = lax.axis_size(COLUMN)
    n_face, n_tile = lax.axis_size(FACE), lax.axis_size(TILE)
    n_plane = lax.axis_size(PLANE)

    def f32(*shape):
        return jax.ShapeDtypeStruct(shape, jnp.float32)

    def in_hbm(x):
        return pltpu.with_memory_space_constraint(x, pltpu.HBM)

    inputs = tuple(in_hbm(x) for x in (air, heat, thick, ground, maps, det, jnp.asarray(lane_tables())))
    params = pltpu.CompilerParams(vmem_limit_bytes=24 * 1024 * 1024)
    share, *rest = pl.pallas_call(
        lambda *refs: column_kernel(n_share, *refs),
        out_shape=(
            f32(n_share, 2 * ROWS, LANES),
            f32(7, levels, ROWS, LANES),
            f32(7, ROWS, LANES),
            jax.ShapeDtypeStruct(inputs[6].shape, inputs[6].dtype),
        ),
        in_specs=[ANY] * 7,
        out_specs=(VMEM,) * 4,
        scratch_shapes=[pltpu.SemaphoreType.DMA((7,))],
        compiler_params=params,
        name="column",
    )(*inputs)
    shared = lax.all_to_all(share, COLUMN, 0, 0, tiled=True)
    dynamics_w, w, packed = pl.pallas_call(
        fields_kernel,
        out_shape=(
            f32(4 * levels * ROWS, LANES),
            f32((edge_rows - 4 * levels) * ROWS, LANES),
            f32(count * ROWS, LANES),
        ),
        in_specs=[VMEM] * 3 + [ANY],
        out_specs=(VMEM,) * 3,
        scratch_shapes=[pltpu.VMEM(tracer.shape, jnp.float32), pltpu.SemaphoreType.DMA((1,))],
        compiler_params=params,
        name="fields",
    )(*rest, in_hbm(tracer))
    wind, far, near, packed, bound = pl.pallas_call(
        lambda *refs: carry_kernel(levels, n_lev, *refs),
        out_shape=(
            f32(2 * levels * ROWS, LANES),
            f32(edge_rows + 2 * ROWS, LANES),
            f32(edge_rows + 2 * ROWS, LANES),
            f32(count * ROWS, LANES),
            f32(n_plane, 1, LANES),
        ),
        in_specs=[VMEM] * 6,
        out_specs=(VMEM,) * 5,
        compiler_params=params,
        name="carry",
    )(shared, dynamics_w, w, packed, maps, det)
    far = swap_pairs(far, FACE, 1)
    near = swap_pairs(near, FACE, 0)
    plane = lax.all_to_all(bound, PLANE, 0, 0, tiled=True)
    stepping_bounds = pl.pallas_call(
        bounds_kernel, out_shape=f32(2), in_specs=[VMEM], out_specs=SMEM, compiler_params=params, name="bounds"
    )(plane)
    sides = jnp.concatenate([packed, far[edge_rows:], near[edge_rows:]], 0)
    inside = swap_pairs(sides, TILE, 0)
    outside = swap_pairs(sides, TILE, 1)
    sums = pl.pallas_call(
        lambda *refs: sum_kernel(levels, n_face, n_tile, *refs),
        out_shape=(f32(*air.shape), f32(*heat.shape), f32(*thick.shape), f32(*tracer.shape)),
        in_specs=[SMEM] * 3 + [VMEM] * 7,
        out_specs=(ANY,) * 4,
        scratch_shapes=[
            pltpu.VMEM((edge_rows, LANES), jnp.float32),
            pltpu.VMEM((edge_rows, LANES), jnp.float32),
            pltpu.VMEM((count, ROWS, LANES), jnp.float32),
            *(pltpu.VMEM(x.shape, jnp.float32) for x in (air, heat, thick, tracer)),
            pltpu.SemaphoreType.DMA((4, levels)),
        ],
        compiler_params=params,
        name="sum",
    )
    air_next, heat_next, thick_next, tracer_next = sums(rotations.reshape(-1), flips.reshape(-1), valences.reshape(-1), w, dynamics_w, wind, far, near, inside, outside)
    return air_next, heat_next, thick_next, tracer_next, stepping_bounds


def solution(mesh):
    face, tile, lev = mesh.shape["face"], mesh.shape["tile"], mesh.shape["lev"]
    inner = min(face, 4)
    split = Mesh(
        mesh.devices.reshape(face // inner, inner, tile // 2, 2, lev),
        ("face_0", "face_1", "tile_0", "tile_1", "lev"),
    )
    level_plane = P("lev", FACE, TILE)
    field_level_plane = P(None, "lev", FACE, TILE)
    return jax.shard_map(
        on_device,
        mesh=split,
        in_specs=(
            field_level_plane, level_plane, level_plane, field_level_plane,
            P(FACE, TILE), P(None, FACE, TILE), P(FACE, TILE), P(), P(), P(),
        ),
        out_specs=(field_level_plane, level_plane, level_plane, field_level_plane, P()),
        check_vma=False,
    )
```
